32 devices in a mesh: gx: 4 (over z), gy: 4 (over y, x), gz: 2 (over core).
Axes of the slice: x: 2, y: 2, z: 4, core: 2. Of those that a mesh axis runs over, the one named last changes fastest.
Arguments:
- pair: bfloat16 [128, 128, 128], P('gx', ('gy', 'gz')), may hold values from -6 to 6
- pair_mask: int32 [128, 128], P('gx', ('gy', 'gz')), may hold values 0 or 1
- in_gain: float32 [128], replicated, may hold values from 0.1 to 1.9
- in_bias: float32 [128], replicated, may hold values from -3 to 3
- proj_weight: bfloat16 [128, 512], replicated, may hold values from -0.5 to 0.5
- gate_weight: bfloat16 [128, 128], replicated, may hold values from -0.5 to 0.5
- out_gain: float32 [128], replicated, may hold values from 0.1 to 1.9
- out_bias: float32 [128], replicated, may hold values from -3 to 3
- out_weight: bfloat16 [128, 128], replicated, may hold values from -0.5 to 0.5
Outputs:
- update: bfloat16 [128, 128, 128], P('gx', ('gy', 'gz'))
The draws below stay inside these ranges and needn't reach their ends.
All inputs are finite; a program needn't handle non-finite values. No bound on the sum of `pair_mask` on one device may be relied on, other than what follows from the above.
Results may differ from the reference program's by a relative error of at most 0.0071.
Values may be sent and summed in bfloat16 or wider, within the bound.
A program may use at most 64 MiB of HBM per device.

```python
import jax
import jax.numpy as jnp
from jax import lax

C = 128
CH = 128
N = 128


def with_ends(array, stream_key, smallest, high):
    spot = [jax.random.randint(jax.random.fold_in(stream_key, axis), (), 0, length) for axis, length in enumerate(array.shape)]
    widest = array.shape.index(max(array.shape))
    beside = spot[:widest] + [(spot[widest] + 1) % array.shape[widest]] + spot[widest + 1:]
    return array.at[tuple(spot)].set(smallest).at[tuple(beside)].set(high)


def block_levels(stream_key, shape, pieces, low, largest):
    loudness = 1.0
    for axis_at, parts in pieces:
        steps = jax.random.uniform(jax.random.fold_in(jax.random.fold_in(stream_key, 6), axis_at), (parts,), jnp.float32, low / len(pieces), largest / len(pieces))
        loudness = loudness * jnp.repeat(jnp.exp(steps), shape[axis_at] // parts).reshape((-1,) + (1,) * (len(shape) - 1 - axis_at))
    return loudness


def gaussian(key, shape, scale, reach, split=(), held_as=jnp.bfloat16):
    result = scale * jax.random.normal(key, shape, jnp.float32)
    if split:
        result = result * block_levels(key, shape, split, -0.22, 0.18)
    return jnp.clip(result, -reach, reach).astype(held_as)


def setup_inputs(seed: int = 0) -> dict:
    splits = jax.random.split(jax.random.key(seed), 10)
    pair = gaussian(splits[0], (N, N, C), 1.0, 6.0, ((0, 4), (1, 8)))
    pair_mask = with_ends((jax.random.randint(splits[1], (N, N), 0, 4) < 3).astype(jnp.int32), jax.random.fold_in(splits[1], 1), 0, 1)
    in_gain = jnp.clip(1.0 + 0.18 * jax.random.normal(splits[2], (C,), jnp.float32), 0.1, 1.9)
    in_bias = gaussian(splits[3], (C,), 0.5, 3.0, (), jnp.float32)
    proj_weight = gaussian(splits[4], (C, 4 * CH), C ** -0.5, 0.5)
    gate_weight = gaussian(splits[5], (C, C), C ** -0.5, 0.5)
    out_gain = jnp.clip(1.0 + 0.18 * jax.random.normal(splits[6], (CH,), jnp.float32), 0.1, 1.9)
    out_bias = gaussian(splits[7], (CH,), 0.5, 3.0, (), jnp.float32)
    out_weight = gaussian(splits[8], (CH, C), CH ** -0.5, 0.5)
    return dict(pair=pair, pair_mask=pair_mask, in_gain=in_gain, in_bias=in_bias, proj_weight=proj_weight, gate_weight=gate_weight, out_gain=out_gain, out_bias=out_bias, out_weight=out_weight)


def normalize(values, gain, bias):
    average = lax.optimization_barrier(jnp.mean(values, axis=-1, keepdims=True))
    centered = values - average
    variance = lax.optimization_barrier(jnp.mean(centered * centered, axis=-1, keepdims=True))
    return centered * lax.rsqrt(variance + 1e-05) * gain + bias

def reference(pair, pair_mask, in_gain, in_bias, proj_weight, gate_weight, out_gain, out_bias, out_weight):
    total = pair.shape[0]
    channels = pair.shape[2]
    hidden = proj_weight.shape[1] // 4
    normed = normalize(pair.astype(jnp.float32), in_gain, in_bias).astype(jnp.bfloat16)
    flat = normed.reshape(total * total, channels)
    projected = jnp.dot(flat, proj_weight, preferred_element_type=jnp.float32).reshape(total, total, 4 * hidden)
    mask_value = pair_mask.astype(jnp.float32)[:, :, None]
    left_side = (jax.nn.sigmoid(projected[:, :, :hidden]) * projected[:, :, hidden:2 * hidden] * mask_value).astype(jnp.bfloat16)
    right_side = (jax.nn.sigmoid(projected[:, :, 2 * hidden:3 * hidden]) * projected[:, :, 3 * hidden:] * mask_value).astype(jnp.bfloat16)
    triangle = jnp.einsum('ikc,jkc->ijc', left_side.astype(jnp.float32), right_side.astype(jnp.float32), precision=lax.Precision.HIGHEST)
    tri_normed = normalize(triangle, out_gain, out_bias).astype(jnp.bfloat16)
    gating = jax.nn.sigmoid(jnp.dot(flat, gate_weight, preferred_element_type=jnp.float32))
    mixed = jnp.dot(tri_normed.reshape(total * total, hidden), out_weight, preferred_element_type=jnp.float32)
    return (gating * mixed).reshape(total, total, channels).astype(jnp.bfloat16)
```

```python
import functools

import jax
import jax.numpy as jnp
from jax import lax
from jax.experimental import pallas as pl
from jax.experimental.pallas import tpu as pltpu
from jax.sharding import PartitionSpec as P

MESH = pl.DeviceIdType.MESH
LANES = 128
EPSILON = 1e-05
PARTS = 2
RIGHT_STEPS = 2
TRI_STEPS = 1


def normalize(values, gain, bias):
    average = jnp.mean(values, axis=-1, keepdims=True)
    centered = values - average
    variance = jnp.mean(centered * centered, axis=-1, keepdims=True)
    return centered * lax.rsqrt(variance + EPSILON) * gain + bias


def project(tile, mask_value, in_gain, in_bias, proj_weight):
    hidden = proj_weight.shape[1] // 4
    normed = normalize(tile.astype(jnp.float32), in_gain, in_bias).astype(jnp.bfloat16)
    projected = jnp.einsum("rwc,cd->rwd", normed, proj_weight, preferred_element_type=jnp.float32)
    left_side = (
        jax.nn.sigmoid(projected[:, :, :hidden]) * projected[:, :, hidden : 2 * hidden] * mask_value
    ).astype(jnp.bfloat16)
    right_side = (
        jax.nn.sigmoid(projected[:, :, 2 * hidden : 3 * hidden])
        * projected[:, :, 3 * hidden :]
        * mask_value
    ).astype(jnp.bfloat16)
    return (normed, left_side, right_side)


def with_collectives(
    pair, pair_mask, in_gain, in_bias, proj_weight, gate_weight, out_gain, out_bias, out_weight
):
    mask_value = pair_mask.astype(jnp.float32)[:, :, None]
    normed, left_side, own_right = project(pair, mask_value, in_gain, in_bias, proj_weight)
    left_slab, right_slab = (
        lax.all_gather(left_side, "gy", axis=1, tiled=True),
        lax.all_gather(own_right, "gy", axis=1, tiled=True),
    )
    every_row = lax.all_gather(own_right, "gx", axis=0, tiled=True)
    row_panel = lax.all_to_all(every_row, "gy", split_axis=0, concat_axis=1, tiled=True)
    summed = lax.psum_scatter(
        jnp.einsum("jkc,ikc->jic", row_panel, left_slab, preferred_element_type=jnp.float32),
        "gz",
        scatter_dimension=0,
        tiled=True,
    )
    triangle = jnp.transpose(summed, (1, 0, 2))
    tri_normed = normalize(triangle, out_gain, out_bias).astype(jnp.bfloat16)
    gating = jax.nn.sigmoid(
        jnp.einsum("rwc,cd->rwd", normed, gate_weight, preferred_element_type=jnp.float32)
    )
    mixed = jnp.einsum("rwh,hc->rwc", tri_normed, out_weight, preferred_element_type=jnp.float32)
    return (gating * mixed).astype(jnp.bfloat16)


def swap_groups(tiles, width):
    tiles = list(tiles)
    group = lax.broadcasted_iota(jnp.int32, tiles[0].shape, 1) // width
    bit = 1
    while bit < len(tiles):
        upper = (group // bit) % 2 == 1
        for a in range(len(tiles)):
            if (a // bit) % 2 == 0:
                low, high = tiles[a], tiles[a + bit]
                tiles[a] = jnp.where(upper, pltpu.roll(high, bit * width, 1), low)
                tiles[a + bit] = jnp.where(upper, high, pltpu.roll(low, LANES - bit * width, 1))
        bit *= 2
    return tiles


def kernel(
    nx,
    ny,
    nz,
    pair_hbm,
    mask_hbm,
    in_gain_hbm,
    in_bias_hbm,
    proj_hbm,
    gate_hbm,
    out_gain_hbm,
    out_bias_hbm,
    out_weight_hbm,
    out_ref,
    right_out,
    left_out,
    tri_out,
    right_in,
    left_in,
    tri_in,
    right_all,
    left_all,
    left_far,
    tri_far,
    spread,
    normed_ref,
    gating_ref,
    right_sems,
    left_sems,
    tri_sems,
    z_send,
    z_recv,
    far_sems,
    far_send,
    pair_ref,
    mask_ref,
    in_gain_ref,
    in_bias_ref,
    proj_ref,
    gate_ref,
    out_gain_ref,
    out_bias_ref,
    out_weight_ref,
    load_sems,
):
    rows, width, channels = pair_ref.shape
    hidden = proj_ref.shape[1] // 4
    plane = ny * nz
    block = hidden // plane
    tiles = rows * width // LANES
    per_tile = rows // tiles
    per_step = tiles // TRI_STEPS
    part = block // PARTS
    x, y, z = lax.axis_index("gx"), lax.axis_index("gy"), lax.axis_index("gz")
    me = y * nz + z
    owners = rows // width
    is_end = jnp.logical_or(x == 0, x == nx - 1)
    is_helper = jnp.logical_or(x == 1, x == nx - 2)
    end = jnp.where(x < nx // 2, 0, nx - 1)
    helper = jnp.where(x < nx // 2, 1, nx - 2)

    def is_left_out(d):
        return jnp.logical_and(is_end, d // owners == nx - 1 - end)


    def peer(t):
        d = lax.rem(me + t, plane)
        return d, (x, d // nz, lax.rem(d, nz))

    arguments = (
        (pair_hbm, pair_ref),
        (mask_hbm, mask_ref),
        (in_gain_hbm, in_gain_ref),
        (in_bias_hbm, in_bias_ref),
        (proj_hbm, proj_ref),
        (gate_hbm, gate_ref),
        (out_gain_hbm, out_gain_ref),
        (out_bias_hbm, out_bias_ref),
        (out_weight_hbm, out_weight_ref),
    )
    loads = [
        pltpu.make_async_copy(held, wanted, load_sems.at[index])
        for index, (held, wanted) in enumerate(arguments)
    ]
    for load in loads:
        load.start()
    barrier = pltpu.get_barrier_semaphore()
    for t in range(1, plane):
        pl.semaphore_signal(barrier, inc=1, device_id=peer(t)[1], device_id_type=MESH)

    @pl.when(x > 0)
    def _():
        pl.semaphore_signal(barrier, inc=1, device_id=(x - 1, y, z), device_id_type=MESH)

    @pl.when(x < nx - 1)
    def _():
        pl.semaphore_signal(barrier, inc=1, device_id=(x + 1, y, z), device_id_type=MESH)

    @pl.when(is_left_out(me))
    def _():
        for t in range(plane):
            d = lax.rem(me + t, plane)
            device = (helper, d // nz, lax.rem(d, nz))
            pl.semaphore_signal(barrier, inc=1, device_id=device, device_id_type=MESH)

    for load in (loads[0], loads[2], loads[3]):
        load.wait()

    def norm(step):
        some = slice(step * rows // RIGHT_STEPS, (step + 1) * rows // RIGHT_STEPS)
        pairs = slice(some.start * width, some.stop * width)
        normed_ref[pairs, :] = normalize(
            pair_ref[some].reshape(-1, channels).astype(jnp.float32), in_gain_ref[...], in_bias_ref[...]
        ).astype(jnp.bfloat16)

    norm(0)

    loads[1].wait()
    row_of = lax.broadcasted_iota(jnp.int32, (rows, rows * width), 1) // width
    choose = (row_of == lax.broadcasted_iota(jnp.int32, row_of.shape, 0)).astype(jnp.bfloat16)
    repeated = jnp.dot(
        mask_ref[...].astype(jnp.float32).astype(jnp.bfloat16), choose, preferred_element_type=jnp.float32
    )
    column_of = lax.broadcasted_iota(jnp.int32, repeated.shape, 1) % width
    own_column = column_of == lax.broadcasted_iota(jnp.int32, repeated.shape, 0)
    mask_row = jnp.sum(jnp.where(own_column, repeated, 0.0), axis=0, keepdims=True)

    def side(weight, target, step, steps):
        for q in range(step * tiles // steps, (step + 1) * tiles // steps):
            lanes = slice(q * LANES, (q + 1) * LANES)
            projected = lax.dot_general(
                weight, normed_ref[lanes, :], (((1,), (1,)), ((), ())), preferred_element_type=jnp.float32
            )
            value = jax.nn.sigmoid(projected[:hidden]) * projected[hidden:] * mask_row[:, lanes]
            target[:, q] = value.astype(jnp.bfloat16).reshape(plane, block, LANES)

    def exchange(source, target, sems, step, steps):
        count = tiles // steps
        copies = []
        for t in range(1, plane):
            d, device = peer(t)
            copies.append(
                pltpu.make_async_remote_copy(
                    src_ref=source.at[d, pl.ds(step * count, count)],
                    dst_ref=target.at[me, pl.ds(step * count, count)],
                    send_sem=sems.at[0, step, t],
                    recv_sem=sems.at[1, step, t],
                    device_id=device,
                    device_id_type=MESH,
                )
            )
            copies[-1].start()
        target[me, step * count : (step + 1) * count] = source[me, step * count : (step + 1) * count]
        return copies

    def gather_sums(source, target, step, steps):
        some = rows // steps
        for index, q in enumerate(range(step * tiles // steps, (step + 1) * tiles // steps)):
            swapped = swap_groups([source[a, q].astype(jnp.float32) for a in range(plane)], width)
            for a in range(per_tile):
                first = step * some * block + index * per_tile + a
                spread[pl.ds(first, block, stride=some), :] = swapped[a]
        target[:, step * some : (step + 1) * some] = (
            spread[step * some * block : (step + 1) * some * block]
            .astype(jnp.bfloat16)
            .reshape(block, some, LANES)
        )

    loads[4].wait()
    right_weight = proj_ref[:, 2 * hidden :].T
    right_copies = []
    for step in range(RIGHT_STEPS):
        if step > 0:
            norm(step)
        side(right_weight, right_out, step, RIGHT_STEPS)
        if step == 0:
            pl.semaphore_wait(
                barrier, jnp.where(is_end, plane, jnp.where(is_helper, plane + 1 + owners, plane + 1))
            )
        right_copies.append(exchange(right_out, right_in, right_sems, step, RIGHT_STEPS))
    side(proj_ref[:, : 2 * hidden].T, left_out, 0, 1)
    left_copies = exchange(left_out, left_in, left_sems, 0, 1)
    loads[5].wait()
    gating_ref[...] = jax.nn.sigmoid(
        jnp.dot(normed_ref[...], gate_ref[...], preferred_element_type=jnp.float32)
    )

    pieces = RIGHT_STEPS * PARTS

    def piece_of(origin, piece):
        some = rows // RIGHT_STEPS
        return right_all.at[
            origin, pl.ds(piece % PARTS * part, part), pl.ds(piece // PARTS * some, some)
        ]

    def pass_on(way, t, piece):
        ahead = x + 1 if way == 0 else x - 1
        origin = x - t if way == 0 else x + t
        part_of = piece_of(origin, piece)
        return pltpu.make_async_remote_copy(
            src_ref=part_of,
            dst_ref=part_of,
            send_sem=z_send.at[way, t, piece],
            recv_sem=z_recv.at[way, t, piece],
            device_id=(ahead, y, z),
            device_id_type=MESH,
        )

    def has_ahead(way):
        return x < nx - 1 if way == 0 else x > 0

    def has_origin(way, t):
        return x >= t if way == 0 else x <= nx - 1 - t

    for step in range(RIGHT_STEPS):
        for copy in right_copies[step]:
            copy.wait_recv()
        gather_sums(right_in, right_all.at[x], step, RIGHT_STEPS)
        for piece in range(step * PARTS, (step + 1) * PARTS):
            for way in range(2):

                @pl.when(has_ahead(way))
                def _():
                    pass_on(way, 0, piece).start()

    for copy in left_copies:
        copy.wait_recv()
    gather_sums(left_in, left_all, 0, 1)

    left_copy = pltpu.make_async_remote_copy(
        src_ref=left_all,
        dst_ref=left_far,
        send_sem=far_sems.at[0],
        recv_sem=far_sems.at[1],
        device_id=(helper, y, z),
        device_id_type=MESH,
    )

    @pl.when(is_end)
    def _():
        left_copy.start()
        right_all[nx - 1 - end] = jnp.zeros(right_all.shape[1:], right_all.dtype)

    for t in range(1, nx - 1):
        for piece in range(pieces):
            for way in range(2):

                @pl.when(has_origin(way, t))
                def _():
                    pltpu.make_async_remote_copy(
                        src_ref=piece_of(x, piece),
                        dst_ref=piece_of(x - t if way == 0 else x + t, piece),
                        send_sem=z_send.at[way, t - 1, piece],
                        recv_sem=z_recv.at[way, t - 1, piece],
                        device_id=(x, y, z),
                        device_id_type=MESH,
                    ).wait_recv()
                    if t < nx - 2:

                        @pl.when(has_ahead(way))
                        def _():
                            pass_on(way, t, piece).start()

    def multiply(left, target, send):
        for c in range(block):
            triangle = lax.dot_general(
                left[c],
                right_all[:, c].reshape(nx * rows, LANES),
                (((1,), (1,)), ((), ())),
                preferred_element_type=jnp.float32,
            )
            spread[pl.ds(c, rows, stride=block), :] = triangle
        for q in range(tiles):
            swapped = swap_groups(
                [spread[pl.ds((q * per_tile + a) * block, block), :] for a in range(per_tile)], width
            )
            for d in range(plane):
                target[d, q] = swapped[d].astype(jnp.bfloat16)
            if (q + 1) % per_step == 0:
                send(q // per_step)

    def far_copy(index, step):
        d = (nx - 1 - end) * owners + index
        return pltpu.make_async_remote_copy(
            src_ref=tri_far.at[d, pl.ds(step * per_step, per_step)],
            dst_ref=tri_in.at[me, pl.ds(step * per_step, per_step)],
            send_sem=far_send.at[step, index],
            recv_sem=tri_sems.at[1, step, lax.rem(d - me + plane, plane)],
            device_id=(end, d // nz, lax.rem(d, nz)),
            device_id_type=MESH,
        )

    def tri_copy(t, step):
        d, device = peer(t)
        return pltpu.make_async_remote_copy(
            src_ref=tri_out.at[d, pl.ds(step * per_step, per_step)],
            dst_ref=tri_in.at[me, pl.ds(step * per_step, per_step)],
            send_sem=tri_sems.at[0, step, t],
            recv_sem=tri_sems.at[1, step, t],
            device_id=device,
            device_id_type=MESH,
        )

    def send_far(step):
        for index in range(owners):
            far_copy(index, step).start()

    def send(step):
        for t in range(1, plane):

            @pl.when(jnp.logical_not(is_left_out(peer(t)[0])))
            def _():
                tri_copy(t, step).start()

    def receive(step):
        @pl.when(is_left_out(me))
        def _():
            tri_copy(0, step).wait_recv()

        for t in range(1, plane):
            tri_copy(t, step).wait_recv()

    @pl.when(is_helper)
    def _():
        left_copy.wait_recv()
        multiply(left_far, tri_far, send_far)

    multiply(left_all, tri_out, send)

    @pl.when(jnp.logical_not(is_left_out(me)))
    def _():
        tri_in[me] = tri_out[me]

    for load in loads[6:]:
        load.wait()
    for q in range(tiles):
        if q % per_step == 0:
            receive(q // per_step)
        lanes = slice(q * LANES, (q + 1) * LANES)
        sums = tri_in[:, q].reshape(hidden, LANES).astype(jnp.float32)
        centered = sums - jnp.mean(sums, axis=0, keepdims=True)
        variance = jnp.mean(centered * centered, axis=0, keepdims=True)
        scaled = (centered * lax.rsqrt(variance + EPSILON)).T
        tri_normed = (scaled * out_gain_ref[...] + out_bias_ref[...]).astype(jnp.bfloat16)
        mixed = jnp.dot(tri_normed, out_weight_ref[...], preferred_element_type=jnp.float32)
        out_ref[q * per_tile : (q + 1) * per_tile] = (
            (gating_ref[lanes, :] * mixed).astype(jnp.bfloat16).reshape(per_tile, width, channels)
        )

    for copy in sum(right_copies, left_copies):
        copy.wait_send()
    for t in range(1, plane):

        @pl.when(jnp.logical_not(is_left_out(peer(t)[0])))
        def _():
            for step in range(TRI_STEPS):
                tri_copy(t, step).wait_send()

    @pl.when(is_helper)
    def _():
        for index in range(owners):
            for step in range(TRI_STEPS):
                far_copy(index, step).wait_send()

    @pl.when(is_end)
    def _():
        left_copy.wait_send()

    for t in range(nx - 2):
        for piece in range(pieces):
            for way in range(2):

                @pl.when(jnp.logical_and(has_ahead(way), has_origin(way, t)))
                def _():
                    pass_on(way, t, piece).wait_send()


def fused(nx, ny, nz, *arguments):
    pair, pair_mask, in_gain, in_bias, proj_weight, gate_weight, out_gain, out_bias, out_weight = arguments
    rows, width, channels = pair.shape
    hidden = proj_weight.shape[1] // 4
    plane = ny * nz
    block = hidden // plane
    tiles = rows * width // LANES
    travelling = pltpu.VMEM((plane, tiles, block, LANES), jnp.bfloat16)
    return pl.pallas_call(
        functools.partial(kernel, nx, ny, nz),
        out_shape=pltpu.VMEM(pair.shape, jnp.bfloat16),
        in_specs=[pl.BlockSpec(memory_space=pltpu.HBM)] * 9,
        out_specs=pl.BlockSpec(memory_space=pltpu.VMEM),
        scratch_shapes=[travelling] * 6
        + [
            pltpu.VMEM((nx, block, rows, LANES), jnp.bfloat16),
            pltpu.VMEM((block, rows, LANES), jnp.bfloat16),
            pltpu.VMEM((block, rows, LANES), jnp.bfloat16),
            travelling,
            pltpu.VMEM((block * rows, LANES), jnp.float32),
            pltpu.VMEM((rows * width, channels), jnp.bfloat16),
            pltpu.VMEM((rows * width, channels), jnp.float32),
        ]
        + [pltpu.SemaphoreType.DMA((2, steps, plane)) for steps in (RIGHT_STEPS, 1, TRI_STEPS)]
        + [pltpu.SemaphoreType.DMA((2, nx - 2, RIGHT_STEPS * PARTS))] * 2
        + [pltpu.SemaphoreType.DMA((2,)), pltpu.SemaphoreType.DMA((TRI_STEPS, rows // width))]
        + [
            pltpu.VMEM(pair.shape, pair.dtype),
            pltpu.VMEM((width, rows), pair_mask.dtype),
            pltpu.VMEM((1, in_gain.size), in_gain.dtype),
            pltpu.VMEM((1, in_bias.size), in_bias.dtype),
            pltpu.VMEM(proj_weight.shape, proj_weight.dtype),
            pltpu.VMEM(gate_weight.shape, gate_weight.dtype),
            pltpu.VMEM((1, out_gain.size), out_gain.dtype),
            pltpu.VMEM((1, out_bias.size), out_bias.dtype),
            pltpu.VMEM(out_weight.shape, out_weight.dtype),
            pltpu.SemaphoreType.DMA((9,)),
        ],
        compiler_params=pltpu.CompilerParams(collective_id=0, has_side_effects=True),
    )(
        pair,
        pair_mask.T,
        in_gain.reshape(1, -1),
        in_bias.reshape(1, -1),
        proj_weight,
        gate_weight,
        out_gain.reshape(1, -1),
        out_bias.reshape(1, -1),
        out_weight,
    )


def solution(mesh):
    nx, ny, nz = mesh.shape["gx"], mesh.shape["gy"], mesh.shape["gz"]
    plane = ny * nz

    def on_device(pair, *others):
        rows, width, channels = pair.shape
        hidden = others[3].shape[1] // 4
        fits = (
            width * plane == LANES
            and rows * nx == LANES
            and rows % plane == 0
            and rows % width == 0
            and rows * width % (RIGHT_STEPS * TRI_STEPS * LANES) == 0
            and nx >= 4
            and channels % LANES == 0
            and hidden % (16 * plane) == 0
        )
        if fits:
            return fused(nx, ny, nz, pair, *others)
        return with_collectives(pair, *others)

    return jax.shard_map(
        on_device,
        mesh=mesh,
        in_specs=(
            P("gx", ("gy", "gz"), None),
            P("gx", ("gy", "gz")),
            P(),
            P(),
            P(),
            P(),
            P(),
            P(),
            P(),
        ),
        out_specs=P("gx", ("gy", "gz"), None),
        check_vma=False,
    )
```

```python
import functools

import jax
import jax.numpy as jnp
from jax import lax
from jax.experimental import pallas as pl
from jax.experimental.pallas import tpu as pltpu
from jax.sharding import PartitionSpec as P

MESH = pl.DeviceIdType.MESH
LANES = 128
EPSILON = 1e-05
RIGHT_STEPS = 2
PAD = 1


def normalize(values, gain, bias):
    average = jnp.mean(values, axis=-1, keepdims=True)
    centered = values - average
    variance = jnp.mean(centered * centered, axis=-1, keepdims=True)
    return centered * lax.rsqrt(variance + EPSILON) * gain + bias


def project(tile, mask_value, in_gain, in_bias, proj_weight):
    hidden = proj_weight.shape[1] // 4
    normed = normalize(tile.astype(jnp.float32), in_gain, in_bias).astype(jnp.bfloat16)
    projected = jnp.einsum("rwc,cd->rwd", normed, proj_weight, preferred_element_type=jnp.float32)
    left_side = (
        jax.nn.sigmoid(projected[:, :, :hidden]) * projected[:, :, hidden : 2 * hidden] * mask_value
    ).astype(jnp.bfloat16)
    right_side = (
        jax.nn.sigmoid(projected[:, :, 2 * hidden : 3 * hidden])
        * projected[:, :, 3 * hidden :]
        * mask_value
    ).astype(jnp.bfloat16)
    return (normed, left_side, right_side)


def with_collectives(
    pair, pair_mask, in_gain, in_bias, proj_weight, gate_weight, out_gain, out_bias, out_weight
):
    mask_value = pair_mask.astype(jnp.float32)[:, :, None]
    normed, left_side, own_right = project(pair, mask_value, in_gain, in_bias, proj_weight)
    left_slab, right_slab = (
        lax.all_gather(left_side, "gy", axis=1, tiled=True),
        lax.all_gather(own_right, "gy", axis=1, tiled=True),
    )
    every_row = lax.all_gather(own_right, "gx", axis=0, tiled=True)
    row_panel = lax.all_to_all(every_row, "gy", split_axis=0, concat_axis=1, tiled=True)
    summed = lax.psum_scatter(
        jnp.einsum("jkc,ikc->jic", row_panel, left_slab, preferred_element_type=jnp.float32),
        "gz",
        scatter_dimension=0,
        tiled=True,
    )
    triangle = jnp.transpose(summed, (1, 0, 2))
    tri_normed = normalize(triangle, out_gain, out_bias).astype(jnp.bfloat16)
    gating = jax.nn.sigmoid(
        jnp.einsum("rwc,cd->rwd", normed, gate_weight, preferred_element_type=jnp.float32)
    )
    mixed = jnp.einsum("rwh,hc->rwc", tri_normed, out_weight, preferred_element_type=jnp.float32)
    return (gating * mixed).astype(jnp.bfloat16)


def swap_groups(tiles, width):
    tiles = list(tiles)
    group = lax.broadcasted_iota(jnp.int32, tiles[0].shape, 1) // width
    bit = 1
    while bit < len(tiles):
        upper = (group // bit) % 2 == 1
        for a in range(len(tiles)):
            if (a // bit) % 2 == 0:
                low, high = tiles[a], tiles[a + bit]
                tiles[a] = jnp.where(upper, pltpu.roll(high, bit * width, 1), low)
                tiles[a + bit] = jnp.where(upper, high, pltpu.roll(low, LANES - bit * width, 1))
        bit *= 2
    return tiles


def kernel(
    nx,
    ny,
    nz,
    pair_hbm,
    mask_hbm,
    in_gain_hbm,
    in_bias_hbm,
    proj_hbm,
    gate_hbm,
    out_gain_hbm,
    out_bias_hbm,
    out_weight_hbm,
    out_ref,
    right_out,
    left_out,
    tri_out,
    right_in,
    left_in,
    tri_in,
    right_all,
    left_all,
    spread,
    normed_ref,
    gating_ref,
    right_send,
    right_recv,
    left_send,
    left_recv,
    tri_send,
    tri_recv,
    pair_ref,
    mask_ref,
    in_gain_ref,
    in_bias_ref,
    proj_ref,
    gate_ref,
    out_gain_ref,
    out_bias_ref,
    out_weight_ref,
    load_sems,
):
    rows, width, channels = pair_ref.shape
    hidden = proj_ref.shape[1] // 4
    plane = ny * nz
    block = hidden // plane
    tiles = rows * width // LANES
    per_tile = rows // tiles
    half = nx // 2
    owners = half * rows // width
    x, y, z = lax.axis_index("gx"), lax.axis_index("gy"), lax.axis_index("gz")
    me = y * nz + z
    last = nx - 1
    is_inner = jnp.logical_or(x == half - 1, x == half)
    beside = x + 1 - 2 * lax.rem(x, 2)
    across = jnp.where(x < half, half, half - 1)
    near = jnp.where(is_inner, beside, x)
    slot = lax.rem(x, 2)
    slot_beside = lax.rem(beside, 2)
    first = lax.rem(x, 2) * half
    owner0 = (x // half) * owners
    holds_left = near == x
    sums_here = (me // owners) * half + x // half == x

    def at(row, d):
        return (row, d // nz, lax.rem(d, nz))

    def turn(t):
        return lax.rem(me + t, plane)

    arguments = (
        (pair_hbm, pair_ref),
        (mask_hbm, mask_ref),
        (in_gain_hbm, in_gain_ref),
        (in_bias_hbm, in_bias_ref),
        (proj_hbm, proj_ref),
        (gate_hbm, gate_ref),
        (out_gain_hbm, out_gain_ref),
        (out_bias_hbm, out_bias_ref),
        (out_weight_hbm, out_weight_ref),
    )
    loads = [
        pltpu.make_async_copy(held, wanted, load_sems.at[index])
        for index, (held, wanted) in enumerate(arguments)
    ]
    for load in loads:
        load.start()
    barrier = pltpu.get_barrier_semaphore()

    def greet(row, start):
        for t in range(start, plane):
            pl.semaphore_signal(barrier, inc=1, device_id=at(row, turn(t)), device_id_type=MESH)

    @pl.when(is_inner)
    def _():
        greet(across, 0)
        greet(jnp.where(x < half, last, 0), 0)

    greet(beside, 0)
    greet(x, 1)

    for load in (loads[0], loads[2], loads[3]):
        load.wait()

    def norm(step):
        some = slice(step * rows // RIGHT_STEPS, (step + 1) * rows // RIGHT_STEPS)
        pairs = slice(some.start * width, some.stop * width)
        normed_ref[pairs, :] = normalize(
            pair_ref[some].reshape(-1, channels).astype(jnp.float32), in_gain_ref[...], in_bias_ref[...]
        ).astype(jnp.bfloat16)

    norm(0)

    loads[1].wait()
    row_of = lax.broadcasted_iota(jnp.int32, (rows, rows * width), 1) // width
    choose = (row_of == lax.broadcasted_iota(jnp.int32, row_of.shape, 0)).astype(jnp.bfloat16)
    repeated = jnp.dot(
        mask_ref[...].astype(jnp.float32).astype(jnp.bfloat16), choose, preferred_element_type=jnp.float32
    )
    column_of = lax.broadcasted_iota(jnp.int32, repeated.shape, 1) % width
    own_column = column_of == lax.broadcasted_iota(jnp.int32, repeated.shape, 0)
    mask_row = jnp.sum(jnp.where(own_column, repeated, 0.0), axis=0, keepdims=True)

    def side(weight, target, step, steps):
        for q in range(step * tiles // steps, (step + 1) * tiles // steps):
            lanes = slice(q * LANES, (q + 1) * LANES)
            projected = lax.dot_general(
                weight, normed_ref[lanes, :], (((1,), (1,)), ((), ())), preferred_element_type=jnp.float32
            )
            value = jax.nn.sigmoid(projected[:hidden]) * projected[hidden:] * mask_row[:, lanes]
            target[:, q] = value.astype(jnp.bfloat16).reshape(plane, block, LANES)

    def part_of(step, steps):
        return pl.ds(step * tiles // steps, tiles // steps)

    def right_copy(far, step, t):
        d = turn(t)
        return pltpu.make_async_remote_copy(
            src_ref=right_out.at[d, part_of(step, RIGHT_STEPS)],
            dst_ref=right_in.at[slot, me, part_of(step, RIGHT_STEPS)],
            send_sem=right_send.at[far],
            recv_sem=right_recv.at[slot],
            device_id=at(beside if far else x, d),
            device_id_type=MESH,
        )

    def left_copy(far, t):
        d = turn(t)
        return pltpu.make_async_remote_copy(
            src_ref=left_out.at[d],
            dst_ref=left_in.at[slot, me],
            send_sem=left_send.at[far],
            recv_sem=left_recv.at[slot],
            device_id=at(across if far else near, d),
            device_id_type=MESH,
        )

    def all_of(held, number, target, send_sem, recv_sem):
        return pltpu.make_async_remote_copy(
            src_ref=held.at[pl.ds(0, number)],
            dst_ref=target.at[pl.ds(0, number)],
            send_sem=send_sem,
            recv_sem=recv_sem,
            device_id=at(beside, me),
            device_id_type=MESH,
        )

    def all_right(which, far, number):
        return all_of(right_out, number, right_in.at[which], right_send.at[far], right_recv.at[which])

    def all_left(which, far, number):
        return all_of(left_out, number, left_in.at[which], left_send.at[far], left_recv.at[which])

    def send_right(far):
        for step in range(RIGHT_STEPS):
            for t in range(0 if far else 1, plane):
                right_copy(far, step, t).start()

    def send_left(far):
        for t in range(1, plane):
            left_copy(far, t).start()
        if far:
            left_copy(far, 0).start()
        else:

            @pl.when(jnp.logical_not(holds_left))
            def _():
                left_copy(far, 0).start()

    def all_greeted():
        pl.semaphore_wait(barrier, 3 * plane - 1)

    loads[4].wait()
    right_weight = proj_ref[:, 2 * hidden :].T
    for step in range(RIGHT_STEPS):
        if step > 0:
            norm(step)
        side(right_weight, right_out, step, RIGHT_STEPS)

    @pl.when(x == last)
    def _():
        all_greeted()
        send_right(1)

    side(proj_ref[:, : 2 * hidden].T, left_out, 0, 1)

    @pl.when(x != last)
    def _():
        all_greeted()

    @pl.when(x == half)
    def _():
        send_right(0)

    send_left(1)

    @pl.when(x != last)
    def _():
        send_right(1)

    @pl.when(x != half)
    def _():
        send_right(0)

    send_left(0)
    right_in[slot, me] = right_out[me]

    @pl.when(holds_left)
    def _():
        left_in[slot, me] = left_out[me]

    loads[5].wait()
    gating_ref[...] = jax.nn.sigmoid(
        jnp.dot(normed_ref[...], gate_ref[...], preferred_element_type=jnp.float32)
    )

    def gather_sums(source, target, step, steps):
        some = rows // steps
        for index, q in enumerate(range(step * tiles // steps, (step + 1) * tiles // steps)):
            swapped = swap_groups([source[a, q].astype(jnp.float32) for a in range(plane)], width)
            for a in range(per_tile):
                spread[pl.ds(index * per_tile + a, block, stride=some + PAD), :] = swapped[a]
        for c in range(block):
            target[c, step * some : (step + 1) * some] = spread[
                pl.ds(c * (some + PAD), some), :
            ].astype(jnp.bfloat16)

    def take_right(which, number):
        all_right(which, 0, number).wait_recv()
        gather_sums(right_in.at[which], right_all.at[which], 0, 1)

    def take_left(which):
        local = jnp.logical_and(holds_left, which == slot)

        @pl.when(local)
        def _():
            all_left(which, 0, plane - 1).wait_recv()

        @pl.when(jnp.logical_not(local))
        def _():
            all_left(which, 0, plane).wait_recv()

        gather_sums(left_in.at[which], left_all, 0, 1)

    take_right(slot, plane - 1)
    take_right(slot_beside, plane)

    def tri_copy(which, index):
        return pltpu.make_async_remote_copy(
            src_ref=tri_out.at[which, index],
            dst_ref=tri_in.at[me],
            send_sem=tri_send,
            recv_sem=tri_recv,
            device_id=at(first + which, owner0 + index),
            device_id_type=MESH,
        )

    def is_mine(which, index):
        return jnp.logical_and(first + which == x, owner0 + index == me)

    low_lanes = lax.broadcasted_iota(jnp.int32, (block, LANES), 1) < owners * width
    for which in range(half):
        take_left(which)
        for c in range(block):
            triangle = lax.dot_general(
                left_all[c],
                right_all[:, c].reshape(half * rows, LANES),
                (((1,), (1,)), ((), ())),
                preferred_element_type=jnp.float32,
            )
            spread[pl.ds(c, rows, stride=block + PAD), : half * rows] = triangle
        for q in range(tiles):
            at_row = [
                spread[pl.ds((q * per_tile + a) * (block + PAD), block), :] for a in range(per_tile)
            ]
            swapped = swap_groups(
                [
                    jnp.where(low_lanes, at_row[a], pltpu.roll(at_row[a + owners], owners * width, 1))
                    for a in range(owners)
                ],
                width,
            )
            for index in range(owners):
                tri_out[which, index, q] = swapped[index].astype(jnp.bfloat16)
        for index in range(owners):

            @pl.when(jnp.logical_not(is_mine(which, index)))
            def _():
                tri_copy(which, index).start()

            @pl.when(is_mine(which, index))
            def _():
                tri_in[me] = tri_out[which, index]

    for load in loads[6:]:
        load.wait()

    def all_sums(number):
        return all_of(tri_in, number, tri_in, tri_send, tri_recv)

    @pl.when(sums_here)
    def _():
        all_sums(plane - 1).wait_recv()

    @pl.when(jnp.logical_not(sums_here))
    def _():
        all_sums(plane).wait_recv()

    for q in range(tiles):
        lanes = slice(q * LANES, (q + 1) * LANES)
        sums = tri_in[:, q].reshape(hidden, LANES).astype(jnp.float32)
        centered = sums - jnp.mean(sums, axis=0, keepdims=True)
        variance = jnp.mean(centered * centered, axis=0, keepdims=True)
        scaled = (centered * lax.rsqrt(variance + EPSILON)).T
        tri_normed = (scaled * out_gain_ref[...] + out_bias_ref[...]).astype(jnp.bfloat16)
        mixed = jnp.dot(tri_normed, out_weight_ref[...], preferred_element_type=jnp.float32)
        out_ref[q * per_tile : (q + 1) * per_tile] = (
            (gating_ref[lanes, :] * mixed).astype(jnp.bfloat16).reshape(per_tile, width, channels)
        )

    all_right(0, 0, plane - 1).wait_send()
    all_right(0, 1, plane).wait_send()
    all_left(0, 1, plane).wait_send()

    @pl.when(holds_left)
    def _():
        all_left(0, 0, plane - 1).wait_send()

    @pl.when(jnp.logical_not(holds_left))
    def _():
        all_left(0, 0, plane).wait_send()

    @pl.when(sums_here)
    def _():
        all_sums(plane - 1).wait_send()

    @pl.when(jnp.logical_not(sums_here))
    def _():
        all_sums(plane).wait_send()


def fused(nx, ny, nz, *arguments):
    pair, pair_mask, in_gain, in_bias, proj_weight, gate_weight, out_gain, out_bias, out_weight = arguments
    rows, width, channels = pair.shape
    hidden = proj_weight.shape[1] // 4
    plane = ny * nz
    block = hidden // plane
    tiles = rows * width // LANES
    half = nx // 2
    owners = half * rows // width
    travelling = (tiles, block, LANES)
    dma = pltpu.SemaphoreType.DMA
    return pl.pallas_call(
        functools.partial(kernel, nx, ny, nz),
        out_shape=pltpu.VMEM(pair.shape, jnp.bfloat16),
        in_specs=[pl.BlockSpec(memory_space=pltpu.HBM)] * 9,
        out_specs=pl.BlockSpec(memory_space=pltpu.VMEM),
        scratch_shapes=[
            pltpu.VMEM((plane, *travelling), jnp.bfloat16),
            pltpu.VMEM((plane, *travelling), jnp.bfloat16),
            pltpu.VMEM((half, owners, *travelling), jnp.bfloat16),
            pltpu.VMEM((2, plane, *travelling), jnp.bfloat16),
            pltpu.VMEM((half, plane, *travelling), jnp.bfloat16),
            pltpu.VMEM((plane, *travelling), jnp.bfloat16),
            pltpu.VMEM((half, block, rows, LANES), jnp.bfloat16),
            pltpu.VMEM((block, rows, LANES), jnp.bfloat16),
            pltpu.VMEM(((block + PAD) * (rows + PAD), LANES), jnp.float32),
            pltpu.VMEM((rows * width, channels), jnp.bfloat16),
            pltpu.VMEM((rows * width, channels), jnp.float32),
            dma((2,)),
            dma((half,)),
            dma((2,)),
            dma((half,)),
            dma,
            dma,
            pltpu.VMEM(pair.shape, pair.dtype),
            pltpu.VMEM((width, rows), pair_mask.dtype),
            pltpu.VMEM((1, in_gain.size), in_gain.dtype),
            pltpu.VMEM((1, in_bias.size), in_bias.dtype),
            pltpu.VMEM(proj_weight.shape, proj_weight.dtype),
            pltpu.VMEM(gate_weight.shape, gate_weight.dtype),
            pltpu.VMEM((1, out_gain.size), out_gain.dtype),
            pltpu.VMEM((1, out_bias.size), out_bias.dtype),
            pltpu.VMEM(out_weight.shape, out_weight.dtype),
            dma((9,)),
        ],
        compiler_params=pltpu.CompilerParams(collective_id=0, has_side_effects=True),
    )(
        pair,
        pair_mask.T,
        in_gain.reshape(1, -1),
        in_bias.reshape(1, -1),
        proj_weight,
        gate_weight,
        out_gain.reshape(1, -1),
        out_bias.reshape(1, -1),
        out_weight,
    )


def solution(mesh):
    nx, ny, nz = mesh.shape["gx"], mesh.shape["gy"], mesh.shape["gz"]
    plane = ny * nz

    def on_device(pair, *others):
        rows, width, channels = pair.shape
        hidden = others[3].shape[1] // 4
        fits = (
            width * plane == LANES
            and rows * nx == LANES
            and rows % width == 0
            and rows * width % (RIGHT_STEPS * LANES) == 0
            and nx == 4
            and channels % LANES == 0
            and hidden % (16 * plane) == 0
        )
        if fits:
            return fused(nx, ny, nz, pair, *others)
        return with_collectives(pair, *others)

    return jax.shard_map(
        on_device,
        mesh=mesh,
        in_specs=(
            P("gx", ("gy", "gz"), None),
            P("gx", ("gy", "gz")),
            P(),
            P(),
            P(),
            P(),
            P(),
            P(),
            P(),
        ),
        out_specs=P("gx", ("gy", "gz"), None),
        check_vma=False,
    )
```

```python
import functools

import jax
import jax.numpy as jnp
from jax import lax
from jax.experimental import pallas as pl
from jax.experimental.pallas import tpu as pltpu
from jax.sharding import PartitionSpec as P

MESH = pl.DeviceIdType.MESH
LANES = 128
EPSILON = 1e-05
CUTS = 2
PAD = 1


def normalize(values, gain, bias):
    average = jnp.mean(values, axis=-1, keepdims=True)
    centered = values - average
    variance = jnp.mean(centered * centered, axis=-1, keepdims=True)
    return centered * lax.rsqrt(variance + EPSILON) * gain + bias


def project(tile, mask_value, in_gain, in_bias, proj_weight):
    hidden = proj_weight.shape[1] // 4
    normed = normalize(tile.astype(jnp.float32), in_gain, in_bias).astype(jnp.bfloat16)
    projected = jnp.einsum("rwc,cd->rwd", normed, proj_weight, preferred_element_type=jnp.float32)
    left_side = (
        jax.nn.sigmoid(projected[:, :, :hidden]) * projected[:, :, hidden : 2 * hidden] * mask_value
    ).astype(jnp.bfloat16)
    right_side = (
        jax.nn.sigmoid(projected[:, :, 2 * hidden : 3 * hidden])
        * projected[:, :, 3 * hidden :]
        * mask_value
    ).astype(jnp.bfloat16)
    return (normed, left_side, right_side)


def with_collectives(
    pair, pair_mask, in_gain, in_bias, proj_weight, gate_weight, out_gain, out_bias, out_weight
):
    mask_value = pair_mask.astype(jnp.float32)[:, :, None]
    normed, left_side, own_right = project(pair, mask_value, in_gain, in_bias, proj_weight)
    left_slab, right_slab = (
        lax.all_gather(left_side, "gy", axis=1, tiled=True),
        lax.all_gather(own_right, "gy", axis=1, tiled=True),
    )
    every_row = lax.all_gather(own_right, "gx", axis=0, tiled=True)
    row_panel = lax.all_to_all(every_row, "gy", split_axis=0, concat_axis=1, tiled=True)
    summed = lax.psum_scatter(
        jnp.einsum("jkc,ikc->jic", row_panel, left_slab, preferred_element_type=jnp.float32),
        "gz",
        scatter_dimension=0,
        tiled=True,
    )
    triangle = jnp.transpose(summed, (1, 0, 2))
    tri_normed = normalize(triangle, out_gain, out_bias).astype(jnp.bfloat16)
    gating = jax.nn.sigmoid(
        jnp.einsum("rwc,cd->rwd", normed, gate_weight, preferred_element_type=jnp.float32)
    )
    mixed = jnp.einsum("rwh,hc->rwc", tri_normed, out_weight, preferred_element_type=jnp.float32)
    return (gating * mixed).astype(jnp.bfloat16)


def swap_groups(tiles, width):
    tiles = list(tiles)
    group = lax.broadcasted_iota(jnp.int32, tiles[0].shape, 1) // width
    bit = 1
    while bit < len(tiles):
        upper = (group // bit) % 2 == 1
        for a in range(len(tiles)):
            if (a // bit) % 2 == 0:
                low, high = tiles[a], tiles[a + bit]
                tiles[a] = jnp.where(upper, pltpu.roll(high, bit * width, 1), low)
                tiles[a + bit] = jnp.where(upper, high, pltpu.roll(low, LANES - bit * width, 1))
        bit *= 2
    return tiles


def kernel(
    nx,
    ny,
    nz,
    pair_hbm,
    mask_hbm,
    in_gain_hbm,
    in_bias_hbm,
    proj_hbm,
    gate_hbm,
    out_gain_hbm,
    out_bias_hbm,
    out_weight_hbm,
    out_ref,
    right_out,
    left_out,
    tri_out,
    right_in,
    left_in,
    tri_in,
    right_all,
    left_all,
    spread,
    sums_at,
    normed_ref,
    gating_ref,
    right_send,
    right_recv,
    left_send,
    left_recv,
    tri_send,
    tri_recv,
    pair_ref,
    mask_ref,
    in_gain_ref,
    in_bias_ref,
    proj_ref,
    gate_ref,
    out_gain_ref,
    out_bias_ref,
    out_weight_ref,
    load_sems,
):
    rows, width, channels = pair_ref.shape
    hidden = proj_ref.shape[1] // 4
    plane = ny * nz
    block = hidden // plane
    tiles = rows * width // LANES
    per_tile = rows // tiles
    cut = block // CUTS
    part = hidden // CUTS
    half = nx // 2
    owners = half * rows // width
    x, y, z = lax.axis_index("gx"), lax.axis_index("gy"), lax.axis_index("gz")
    me = y * nz + z
    last = nx - 1
    is_inner = jnp.logical_or(x == half - 1, x == half)
    beside = x + 1 - 2 * lax.rem(x, 2)
    across = jnp.where(x < half, half, half - 1)
    near = jnp.where(is_inner, beside, x)
    slot = lax.rem(x, 2)
    slot_beside = lax.rem(beside, 2)
    first = lax.rem(x, 2) * half
    owner0 = (x // half) * owners
    holds_left = near == x
    sums_here = (me // owners) * half + x // half == x

    def at(row, d):
        return (row, d // nz, lax.rem(d, nz))

    def turn(t):
        return lax.rem(me + t, plane)

    arguments = (
        (pair_hbm, pair_ref),
        (mask_hbm, mask_ref),
        (in_gain_hbm, in_gain_ref),
        (in_bias_hbm, in_bias_ref),
        (proj_hbm, proj_ref),
        (gate_hbm, gate_ref),
        (out_gain_hbm, out_gain_ref),
        (out_bias_hbm, out_bias_ref),
        (out_weight_hbm, out_weight_ref),
    )
    loads = [
        pltpu.make_async_copy(held, wanted, load_sems.at[index])
        for index, (held, wanted) in enumerate(arguments)
    ]
    for load in loads:
        load.start()
    barrier = pltpu.get_barrier_semaphore()

    def greet(row, start):
        for t in range(start, plane):
            pl.semaphore_signal(barrier, inc=1, device_id=at(row, turn(t)), device_id_type=MESH)

    @pl.when(is_inner)
    def _():
        greet(across, 0)
        greet(jnp.where(x < half, last, 0), 0)

    greet(beside, 0)
    greet(x, 1)

    for load in (loads[0], loads[2], loads[3]):
        load.wait()

    normed_ref[...] = normalize(
        pair_ref[...].reshape(-1, channels).astype(jnp.float32), in_gain_ref[...], in_bias_ref[...]
    ).astype(jnp.bfloat16)
    loads[1].wait()
    row_of = lax.broadcasted_iota(jnp.int32, (rows, rows * width), 1) // width
    choose = (row_of == lax.broadcasted_iota(jnp.int32, row_of.shape, 0)).astype(jnp.bfloat16)
    repeated = jnp.dot(
        mask_ref[...].astype(jnp.float32).astype(jnp.bfloat16), choose, preferred_element_type=jnp.float32
    )
    column_of = lax.broadcasted_iota(jnp.int32, repeated.shape, 1) % width
    own_column = column_of == lax.broadcasted_iota(jnp.int32, repeated.shape, 0)
    mask_row = jnp.sum(jnp.where(own_column, repeated, 0.0), axis=0, keepdims=True)

    def side(base, target, h):
        gates = proj_ref[:, base + h * part : base + (h + 1) * part]
        values = proj_ref[:, base + hidden + h * part : base + hidden + (h + 1) * part]
        weight = jnp.concatenate([gates, values], axis=1).T
        for q in range(tiles):
            lanes = slice(q * LANES, (q + 1) * LANES)
            projected = lax.dot_general(
                weight, normed_ref[lanes, :], (((1,), (1,)), ((), ())), preferred_element_type=jnp.float32
            )
            value = jax.nn.sigmoid(projected[:part]) * projected[part:] * mask_row[:, lanes]
            target[h, :, q] = value.astype(jnp.bfloat16).reshape(plane, cut, LANES)

    def right_copy(far, h, t):
        d = turn(t)
        return pltpu.make_async_remote_copy(
            src_ref=right_out.at[h, d],
            dst_ref=right_in.at[slot, h, me],
            send_sem=right_send.at[far],
            recv_sem=right_recv.at[slot, h],
            device_id=at(beside if far else x, d),
            device_id_type=MESH,
        )

    def left_copy(far, h, t):
        d = turn(t)
        return pltpu.make_async_remote_copy(
            src_ref=left_out.at[h, d],
            dst_ref=left_in.at[slot, h, me],
            send_sem=left_send.at[far],
            recv_sem=left_recv.at[slot, h],
            device_id=at(across if far else near, d),
            device_id_type=MESH,
        )

    def arrived(target, sem, number):
        whole = target.at[pl.ds(0, number)]
        pltpu.make_async_remote_copy(
            src_ref=whole,
            dst_ref=whole,
            send_sem=tri_send,
            recv_sem=sem,
            device_id=at(beside, me),
            device_id_type=MESH,
        ).wait_recv()

    def departed(held, sem, number):
        whole = held.at[:, pl.ds(0, number)]
        pltpu.make_async_remote_copy(
            src_ref=whole,
            dst_ref=whole,
            send_sem=sem,
            recv_sem=tri_recv.at[0],
            device_id=at(beside, me),
            device_id_type=MESH,
        ).wait_send()

    def send_right(far, h):
        for t in range(0 if far else 1, plane):
            right_copy(far, h, t).start()

    def send_left(far, h):
        for t in range(1, plane):
            left_copy(far, h, t).start()
        if far:
            left_copy(far, h, 0).start()
        else:

            @pl.when(jnp.logical_not(holds_left))
            def _():
                left_copy(far, h, 0).start()

    def all_greeted():
        pl.semaphore_wait(barrier, 3 * plane - 1)

    loads[4].wait()
    for h in range(CUTS):
        side(2 * hidden, right_out, h)

        @pl.when(x == last)
        def _():
            if h == 0:
                all_greeted()
            send_right(1, h)

        side(0, left_out, h)

        @pl.when(x != last)
        def _():
            if h == 0:
                all_greeted()

        @pl.when(x == half)
        def _():
            send_right(0, h)

        send_left(1, h)

        @pl.when(x != last)
        def _():
            send_right(1, h)

        @pl.when(x != half)
        def _():
            send_right(0, h)

        send_left(0, h)
        right_in[slot, h, me] = right_out[h, me]

        @pl.when(holds_left)
        def _():
            left_in[slot, h, me] = left_out[h, me]

    loads[5].wait()
    gating_ref[...] = jax.nn.sigmoid(
        jnp.dot(normed_ref[...], gate_ref[...], preferred_element_type=jnp.float32)
    )

    def gather_sums(source, target, at_rows):
        for q in range(tiles):
            swapped = swap_groups([source[a, q].astype(jnp.float32) for a in range(plane)], width)
            for a in range(per_tile):
                at_rows[pl.ds(q * per_tile + a, cut, stride=rows + PAD), :] = swapped[a]
        for c in range(cut):
            target[c] = at_rows[pl.ds(c * (rows + PAD), rows), :].astype(jnp.bfloat16)

    def left_arrived(which, h):
        local = jnp.logical_and(holds_left, which == slot)

        @pl.when(local)
        def _():
            arrived(left_in.at[which, h], left_recv.at[which, h], plane - 1)

        @pl.when(jnp.logical_not(local))
        def _():
            arrived(left_in.at[which, h], left_recv.at[which, h], plane)

    def tri_copy(which, h, index):
        return pltpu.make_async_remote_copy(
            src_ref=tri_out.at[h, which, index],
            dst_ref=tri_in.at[h, me],
            send_sem=tri_send,
            recv_sem=tri_recv.at[h],
            device_id=at(first + which, owner0 + index),
            device_id_type=MESH,
        )

    def is_mine(which, index):
        return jnp.logical_and(first + which == x, owner0 + index == me)

    low_lanes = lax.broadcasted_iota(jnp.int32, (cut, LANES), 1) < owners * width
    for h in range(CUTS):
        arrived(right_in.at[slot, h], right_recv.at[slot, h], plane - 1)
        arrived(right_in.at[slot_beside, h], right_recv.at[slot_beside, h], plane)
        for which in range(half):
            left_arrived(which, h)
        for which in range(half):
            gather_sums(right_in.at[which, h], right_all.at[which], spread.at[which])
            gather_sums(left_in.at[which, h], left_all.at[which], spread.at[half + which])
        for c in range(cut):
            triangle = lax.dot_general(
                left_all[:, c].reshape(half * rows, LANES),
                right_all[:, c].reshape(half * rows, LANES),
                (((1,), (1,)), ((), ())),
                preferred_element_type=jnp.float32,
            )
            for which in range(half):
                sums_at[which, pl.ds(c, rows, stride=cut + PAD), : half * rows] = triangle[
                    which * rows : (which + 1) * rows
                ]
        for which in range(half):
            for q in range(tiles):
                at_row = [
                    sums_at[which, pl.ds((q * per_tile + a) * (cut + PAD), cut), :] for a in range(per_tile)
                ]
                swapped = swap_groups(
                    [
                        jnp.where(low_lanes, at_row[a], pltpu.roll(at_row[a + owners], owners * width, 1))
                        for a in range(owners)
                    ],
                    width,
                )
                for index in range(owners):
                    tri_out[h, which, index, q] = swapped[index].astype(jnp.bfloat16)
        for which in range(half):
            for index in range(owners):

                @pl.when(jnp.logical_not(is_mine(which, index)))
                def _():
                    tri_copy(which, h, index).start()

                @pl.when(is_mine(which, index))
                def _():
                    tri_in[h, me] = tri_out[h, which, index]

    for load in loads[6:]:
        load.wait()

    @pl.when(sums_here)
    def _():
        for h in range(CUTS):
            arrived(tri_in.at[h], tri_recv.at[h], plane - 1)

    @pl.when(jnp.logical_not(sums_here))
    def _():
        for h in range(CUTS):
            arrived(tri_in.at[h], tri_recv.at[h], plane)

    for q in range(tiles):
        lanes = slice(q * LANES, (q + 1) * LANES)
        sums = tri_in[:, :, q].astype(jnp.float32).reshape(hidden, LANES)
        centered = sums - jnp.mean(sums, axis=0, keepdims=True)
        variance = jnp.mean(centered * centered, axis=0, keepdims=True)
        scaled = (centered * lax.rsqrt(variance + EPSILON)).T
        tri_normed = (scaled * out_gain_ref[...] + out_bias_ref[...]).astype(jnp.bfloat16)
        mixed = jnp.dot(tri_normed, out_weight_ref[...], preferred_element_type=jnp.float32)
        out_ref[q * per_tile : (q + 1) * per_tile] = (
            (gating_ref[lanes, :] * mixed).astype(jnp.bfloat16).reshape(per_tile, width, channels)
        )

    departed(right_out, right_send.at[0], plane - 1)
    departed(right_out, right_send.at[1], plane)
    departed(left_out, left_send.at[1], plane)

    @pl.when(holds_left)
    def _():
        departed(left_out, left_send.at[0], plane - 1)

    @pl.when(jnp.logical_not(holds_left))
    def _():
        departed(left_out, left_send.at[0], plane)

    @pl.when(sums_here)
    def _():
        departed(tri_in, tri_send, plane - 1)

    @pl.when(jnp.logical_not(sums_here))
    def _():
        departed(tri_in, tri_send, plane)


def fused(nx, ny, nz, *arguments):
    pair, pair_mask, in_gain, in_bias, proj_weight, gate_weight, out_gain, out_bias, out_weight = arguments
    rows, width, channels = pair.shape
    hidden = proj_weight.shape[1] // 4
    plane = ny * nz
    block = hidden // plane
    tiles = rows * width // LANES
    half = nx // 2
    owners = half * rows // width
    cut = block // CUTS
    travelling = (plane, tiles, cut, LANES)
    dma = pltpu.SemaphoreType.DMA
    return pl.pallas_call(
        functools.partial(kernel, nx, ny, nz),
        out_shape=pltpu.VMEM(pair.shape, jnp.bfloat16),
        in_specs=[pl.BlockSpec(memory_space=pltpu.HBM)] * 9,
        out_specs=pl.BlockSpec(memory_space=pltpu.VMEM),
        scratch_shapes=[
            pltpu.VMEM((CUTS, *travelling), jnp.bfloat16),
            pltpu.VMEM((CUTS, *travelling), jnp.bfloat16),
            pltpu.VMEM((CUTS, half, owners, *travelling[1:]), jnp.bfloat16),
            pltpu.VMEM((half, CUTS, *travelling), jnp.bfloat16),
            pltpu.VMEM((half, CUTS, *travelling), jnp.bfloat16),
            pltpu.VMEM((CUTS, *travelling), jnp.bfloat16),
            pltpu.VMEM((half, cut, rows, LANES), jnp.bfloat16),
            pltpu.VMEM((half, cut, rows, LANES), jnp.bfloat16),
            pltpu.VMEM((2 * half, cut * (rows + PAD), LANES), jnp.float32),
            pltpu.VMEM((half, rows * (cut + PAD), LANES), jnp.float32),
            pltpu.VMEM((rows * width, channels), jnp.bfloat16),
            pltpu.VMEM((rows * width, channels), jnp.float32),
            dma((2,)),
            dma((half, CUTS)),
            dma((2,)),
            dma((half, CUTS)),
            dma,
            dma((CUTS,)),
            pltpu.VMEM(pair.shape, pair.dtype),
            pltpu.VMEM((width, rows), pair_mask.dtype),
            pltpu.VMEM((1, in_gain.size), in_gain.dtype),
            pltpu.VMEM((1, in_bias.size), in_bias.dtype),
            pltpu.VMEM(proj_weight.shape, proj_weight.dtype),
            pltpu.VMEM(gate_weight.shape, gate_weight.dtype),
            pltpu.VMEM((1, out_gain.size), out_gain.dtype),
            pltpu.VMEM((1, out_bias.size), out_bias.dtype),
            pltpu.VMEM(out_weight.shape, out_weight.dtype),
            dma((9,)),
        ],
        compiler_params=pltpu.CompilerParams(collective_id=0, has_side_effects=True),
    )(
        pair,
        pair_mask.T,
        in_gain.reshape(1, -1),
        in_bias.reshape(1, -1),
        proj_weight,
        gate_weight,
        out_gain.reshape(1, -1),
        out_bias.reshape(1, -1),
        out_weight,
    )


def solution(mesh):
    nx, ny, nz = mesh.shape["gx"], mesh.shape["gy"], mesh.shape["gz"]
    plane = ny * nz

    def on_device(pair, *others):
        rows, width, channels = pair.shape
        hidden = others[3].shape[1] // 4
        fits = (
            width * plane == LANES
            and rows * nx == LANES
            and rows % width == 0
            and rows * width % LANES == 0
            and nx == 4
            and channels % LANES == 0
            and hidden % (8 * CUTS * plane) == 0
        )
        if fits:
            return fused(nx, ny, nz, pair, *others)
        return with_collectives(pair, *others)

    return jax.shard_map(
        on_device,
        mesh=mesh,
        in_specs=(
            P("gx", ("gy", "gz"), None),
            P("gx", ("gy", "gz")),
            P(),
            P(),
            P(),
            P(),
            P(),
            P(),
            P(),
        ),
        out_specs=P("gx", ("gy", "gz"), None),
        check_vma=False,
    )
```

```python
import functools

import jax
import jax.numpy as jnp
from jax import lax
from jax.experimental import pallas as pl
from jax.experimental.pallas import tpu as pltpu
from jax.sharding import PartitionSpec as P

MESH = pl.DeviceIdType.MESH
LANES = 128
EPSILON = 1e-05
CUTS = 2
PAD = 1


def normalize(values, gain, bias):
    average = jnp.mean(values, axis=-1, keepdims=True)
    centered = values - average
    variance = jnp.mean(centered * centered, axis=-1, keepdims=True)
    return centered * lax.rsqrt(variance + EPSILON) * gain + bias


def project(tile, mask_value, in_gain, in_bias, proj_weight):
    hidden = proj_weight.shape[1] // 4
    normed = normalize(tile.astype(jnp.float32), in_gain, in_bias).astype(jnp.bfloat16)
    projected = jnp.einsum("rwc,cd->rwd", normed, proj_weight, preferred_element_type=jnp.float32)
    left_side = (
        jax.nn.sigmoid(projected[:, :, :hidden]) * projected[:, :, hidden : 2 * hidden] * mask_value
    ).astype(jnp.bfloat16)
    right_side = (
        jax.nn.sigmoid(projected[:, :, 2 * hidden : 3 * hidden])
        * projected[:, :, 3 * hidden :]
        * mask_value
    ).astype(jnp.bfloat16)
    return (normed, left_side, right_side)


def with_collectives(
    pair, pair_mask, in_gain, in_bias, proj_weight, gate_weight, out_gain, out_bias, out_weight
):
    mask_value = pair_mask.astype(jnp.float32)[:, :, None]
    normed, left_side, own_right = project(pair, mask_value, in_gain, in_bias, proj_weight)
    left_slab, right_slab = (
        lax.all_gather(left_side, "gy", axis=1, tiled=True),
        lax.all_gather(own_right, "gy", axis=1, tiled=True),
    )
    every_row = lax.all_gather(own_right, "gx", axis=0, tiled=True)
    row_panel = lax.all_to_all(every_row, "gy", split_axis=0, concat_axis=1, tiled=True)
    summed = lax.psum_scatter(
        jnp.einsum("jkc,ikc->jic", row_panel, left_slab, preferred_element_type=jnp.float32),
        "gz",
        scatter_dimension=0,
        tiled=True,
    )
    triangle = jnp.transpose(summed, (1, 0, 2))
    tri_normed = normalize(triangle, out_gain, out_bias).astype(jnp.bfloat16)
    gating = jax.nn.sigmoid(
        jnp.einsum("rwc,cd->rwd", normed, gate_weight, preferred_element_type=jnp.float32)
    )
    mixed = jnp.einsum("rwh,hc->rwc", tri_normed, out_weight, preferred_element_type=jnp.float32)
    return (gating * mixed).astype(jnp.bfloat16)


def swap_groups(tiles, width):
    tiles = list(tiles)
    group = lax.broadcasted_iota(jnp.int32, tiles[0].shape, 1) // width
    bit = 1
    while bit < len(tiles):
        upper = (group // bit) % 2 == 1
        for a in range(len(tiles)):
            if (a // bit) % 2 == 0:
                low, high = tiles[a], tiles[a + bit]
                tiles[a] = jnp.where(upper, pltpu.roll(high, bit * width, 1), low)
                tiles[a + bit] = jnp.where(upper, high, pltpu.roll(low, LANES - bit * width, 1))
        bit *= 2
    return tiles


def kernel(
    nx,
    ny,
    nz,
    pair_hbm,
    mask_hbm,
    in_gain_hbm,
    in_bias_hbm,
    proj_hbm,
    gate_hbm,
    out_gain_hbm,
    out_bias_hbm,
    out_weight_hbm,
    out_ref,
    right_out,
    left_out,
    tri_out,
    right_in,
    left_in,
    tri_in,
    right_all,
    left_all,
    spread,
    sums_at,
    normed_ref,
    gating_ref,
    right_send,
    right_recv,
    left_send,
    left_recv,
    tri_send,
    tri_recv,
    above_in,
    pair_ref,
    mask_ref,
    in_gain_ref,
    in_bias_ref,
    proj_ref,
    gate_ref,
    out_gain_ref,
    out_bias_ref,
    out_weight_ref,
    load_sems,
):
    rows, width, channels = pair_ref.shape
    hidden = proj_ref.shape[1] // 4
    plane = ny * nz
    block = hidden // plane
    tiles = rows * width // LANES
    per_tile = rows // tiles
    cut = block // CUTS
    part = hidden // CUTS
    half = nx // 2
    owners = half * rows // width
    x, y, z = lax.axis_index("gx"), lax.axis_index("gy"), lax.axis_index("gz")
    me = y * nz + z
    last = nx - 1
    is_inner = jnp.logical_or(x == half - 1, x == half)
    beside = x + 1 - 2 * lax.rem(x, 2)
    across = jnp.where(x < half, half, half - 1)
    near = jnp.where(is_inner, beside, x)
    slot = lax.rem(x, 2)
    slot_beside = lax.rem(beside, 2)
    first = lax.rem(x, 2) * half
    owner0 = (x // half) * owners
    holds_left = near == x
    sums_here = (me // owners) * half + x // half == x

    def at(row, d):
        return (row, d // nz, lax.rem(d, nz))

    def turn(t):
        return lax.rem(me + t, plane)

    barrier = pltpu.get_barrier_semaphore()

    def greet(row, start):
        for t in range(start, plane):
            pl.semaphore_signal(barrier, inc=1, device_id=at(row, turn(t)), device_id_type=MESH)

    @pl.when(x < half)
    def _():
        greet(x + 1, 0)

    @pl.when(x == half)
    def _():
        greet(x - 1, 0)

    @pl.when(is_inner)
    def _():
        greet(last, 0)

    greet(x, 1)

    arguments = (
        (pair_hbm, pair_ref),
        (mask_hbm, mask_ref),
        (in_gain_hbm, in_gain_ref),
        (in_bias_hbm, in_bias_ref),
        (proj_hbm, proj_ref),
        (gate_hbm, gate_ref),
        (out_gain_hbm, out_gain_ref),
        (out_bias_hbm, out_bias_ref),
        (out_weight_hbm, out_weight_ref),
    )
    loads = [
        pltpu.make_async_copy(held, wanted, load_sems.at[index])
        for index, (held, wanted) in enumerate(arguments)
    ]
    for load in loads:
        load.start()
    for load in (loads[0], loads[2], loads[3]):
        load.wait()

    normed_ref[...] = normalize(
        pair_ref[...].reshape(-1, channels).astype(jnp.float32), in_gain_ref[...], in_bias_ref[...]
    ).astype(jnp.bfloat16)
    loads[1].wait()
    row_of = lax.broadcasted_iota(jnp.int32, (rows, rows * width), 1) // width
    choose = (row_of == lax.broadcasted_iota(jnp.int32, row_of.shape, 0)).astype(jnp.bfloat16)
    repeated = jnp.dot(
        mask_ref[...].astype(jnp.float32).astype(jnp.bfloat16), choose, preferred_element_type=jnp.float32
    )
    column_of = lax.broadcasted_iota(jnp.int32, repeated.shape, 1) % width
    own_column = column_of == lax.broadcasted_iota(jnp.int32, repeated.shape, 0)
    mask_row = jnp.sum(jnp.where(own_column, repeated, 0.0), axis=0, keepdims=True)

    def side(base, target, h):
        gates = proj_ref[:, base + h * part : base + (h + 1) * part]
        values = proj_ref[:, base + hidden + h * part : base + hidden + (h + 1) * part]
        weight = jnp.concatenate([gates, values], axis=1).T
        for q in range(tiles):
            lanes = slice(q * LANES, (q + 1) * LANES)
            projected = lax.dot_general(
                weight, normed_ref[lanes, :], (((1,), (1,)), ((), ())), preferred_element_type=jnp.float32
            )
            value = jax.nn.sigmoid(projected[:part]) * projected[part:] * mask_row[:, lanes]
            target[h, :, q] = value.astype(jnp.bfloat16).reshape(plane, cut, LANES)

    def right_copy(far, h, t):
        d = turn(t)
        return pltpu.make_async_remote_copy(
            src_ref=right_out.at[h, d],
            dst_ref=right_in.at[slot, h, me],
            send_sem=right_send.at[far],
            recv_sem=right_recv.at[slot, h],
            device_id=at(beside if far else x, d),
            device_id_type=MESH,
        )

    def left_copy(far, h, t):
        d = turn(t)
        return pltpu.make_async_remote_copy(
            src_ref=left_out.at[h, d],
            dst_ref=left_in.at[slot, h, me],
            send_sem=left_send.at[far],
            recv_sem=left_recv.at[slot, h],
            device_id=at(across if far else near, d),
            device_id_type=MESH,
        )

    def arrived(target, sem, number):
        whole = target.at[pl.ds(0, number)]
        pltpu.make_async_remote_copy(
            src_ref=whole,
            dst_ref=whole,
            send_sem=tri_send,
            recv_sem=sem,
            device_id=at(beside, me),
            device_id_type=MESH,
        ).wait_recv()

    def departed(held, sem, number):
        whole = held.at[:, pl.ds(0, number)]
        pltpu.make_async_remote_copy(
            src_ref=whole,
            dst_ref=whole,
            send_sem=sem,
            recv_sem=tri_recv.at[0],
            device_id=at(beside, me),
            device_id_type=MESH,
        ).wait_send()

    def send_right(far, h):
        for t in range(0 if far else 1, plane):
            right_copy(far, h, t).start()

    def send_left(far, h):
        for t in range(1, plane):
            left_copy(far, h, t).start()
        if far:
            left_copy(far, h, 0).start()
        else:

            @pl.when(jnp.logical_not(holds_left))
            def _():
                left_copy(far, h, 0).start()

    def all_greeted():
        others = jnp.where(x == 0, 0, jnp.where(x == half, 1, 2))
        pl.semaphore_wait(barrier, plane - 1 + plane * others)

    def tell():
        pl.semaphore_signal(above_in, inc=1, device_id=at(x - 1, me), device_id_type=MESH)

    def told():
        pl.semaphore_wait(above_in, 1)

    loads[4].wait()
    side(2 * hidden, right_out, 0)

    @pl.when(x == last)
    def _():
        all_greeted()
        tell()
        send_right(1, 0)

    side(0, left_out, 0)

    @pl.when(x == 0)
    def _():
        all_greeted()
        send_right(0, 0)
        send_left(0, 0)

    @pl.when(x == half - 1)
    def _():
        all_greeted()
        tell()
        send_left(1, 0)
        send_left(0, 0)
        send_right(0, 0)
        send_right(1, 0)

    @pl.when(x == half)
    def _():
        all_greeted()
        send_right(0, 0)
        send_left(1, 0)

    @pl.when(x == last)
    def _():
        send_left(1, 0)
        send_right(0, 0)
        send_left(0, 0)

    side(2 * hidden, right_out, 1)
    side(0, left_out, 1)

    @pl.when(x == 0)
    def _():
        send_right(0, 1)
        send_left(0, 1)
        told()
        send_left(1, 0)
        send_right(1, 0)
        send_left(1, 1)
        send_right(1, 1)

    @pl.when(x == half - 1)
    def _():
        send_left(1, 1)
        send_left(0, 1)
        send_right(0, 1)
        send_right(1, 1)

    @pl.when(x == half)
    def _():
        send_right(0, 1)
        send_left(1, 1)
        told()
        send_right(1, 0)
        send_left(0, 0)
        send_right(1, 1)
        send_left(0, 1)

    @pl.when(x == last)
    def _():
        send_right(1, 1)
        send_left(1, 1)
        send_right(0, 1)
        send_left(0, 1)

    for h in range(CUTS):
        right_in[slot, h, me] = right_out[h, me]

        @pl.when(holds_left)
        def _():
            left_in[slot, h, me] = left_out[h, me]

    loads[5].wait()
    gating_ref[...] = jax.nn.sigmoid(
        jnp.dot(normed_ref[...], gate_ref[...], preferred_element_type=jnp.float32)
    )

    def gather_sums(source, target, at_rows):
        for q in range(tiles):
            swapped = swap_groups([source[a, q].astype(jnp.float32) for a in range(plane)], width)
            for a in range(per_tile):
                at_rows[pl.ds(q * per_tile + a, cut, stride=rows + PAD), :] = swapped[a]
        for c in range(cut):
            target[c] = at_rows[pl.ds(c * (rows + PAD), rows), :].astype(jnp.bfloat16)

    def left_arrived(which, h):
        local = jnp.logical_and(holds_left, which == slot)

        @pl.when(local)
        def _():
            arrived(left_in.at[which, h], left_recv.at[which, h], plane - 1)

        @pl.when(jnp.logical_not(local))
        def _():
            arrived(left_in.at[which, h], left_recv.at[which, h], plane)

    def tri_copy(which, h, index):
        return pltpu.make_async_remote_copy(
            src_ref=tri_out.at[h, which, index],
            dst_ref=tri_in.at[h, me],
            send_sem=tri_send,
            recv_sem=tri_recv.at[h],
            device_id=at(first + which, owner0 + index),
            device_id_type=MESH,
        )

    def is_mine(which, index):
        return jnp.logical_and(first + which == x, owner0 + index == me)

    lane = lax.broadcasted_iota(jnp.int32, (cut, LANES), 1)
    fewer = owners // half
    for h in range(CUTS):
        for which in range(half):
            left_arrived(which, h)
        for column in range(half):

            @pl.when(slot == column)
            def _():
                arrived(right_in.at[column, h], right_recv.at[column, h], plane - 1)

            @pl.when(slot != column)
            def _():
                arrived(right_in.at[column, h], right_recv.at[column, h], plane)

            gather_sums(right_in.at[column, h], right_all.at[column], spread.at[column])
            if column == 0:
                for which in range(half):
                    gather_sums(left_in.at[which, h], left_all.at[which], spread.at[half + which])
            for c in range(cut):
                triangle = lax.dot_general(
                    left_all[:, c].reshape(half * rows, LANES),
                    right_all[column, c],
                    (((1,), (1,)), ((), ())),
                    preferred_element_type=jnp.float32,
                )
                for which in range(half):
                    sums_at[which, pl.ds(c, rows, stride=cut + PAD), :rows] = triangle[
                        which * rows : (which + 1) * rows
                    ]
            for which in range(half):
                for q in range(tiles):
                    at_row = [
                        sums_at[which, pl.ds((q * per_tile + a) * (cut + PAD), cut), :]
                        for a in range(per_tile)
                    ]
                    packed = []
                    for a in range(fewer):
                        lanes_of = at_row[a]
                        for g in range(1, per_tile // fewer):
                            moved = pltpu.roll(at_row[a + g * fewer], g * fewer * width, 1)
                            lanes_of = jnp.where(lane < g * fewer * width, lanes_of, moved)
                        packed.append(lanes_of)
                    swapped = swap_groups(packed, width)
                    for index in range(fewer):
                        tri_out[h, which, column * fewer + index, q] = swapped[index].astype(jnp.bfloat16)
            for index in range(column * fewer, (column + 1) * fewer):
                for which in range(half):

                    @pl.when(jnp.logical_not(is_mine(which, index)))
                    def _():
                        tri_copy(which, h, index).start()

                    @pl.when(is_mine(which, index))
                    def _():
                        tri_in[h, me] = tri_out[h, which, index]

    for load in loads[6:]:
        load.wait()

    @pl.when(sums_here)
    def _():
        for h in range(CUTS):
            arrived(tri_in.at[h], tri_recv.at[h], plane - 1)

    @pl.when(jnp.logical_not(sums_here))
    def _():
        for h in range(CUTS):
            arrived(tri_in.at[h], tri_recv.at[h], plane)

    for q in range(tiles):
        lanes = slice(q * LANES, (q + 1) * LANES)
        sums = tri_in[:, :, q].astype(jnp.float32).reshape(hidden, LANES)
        centered = sums - jnp.mean(sums, axis=0, keepdims=True)
        variance = jnp.mean(centered * centered, axis=0, keepdims=True)
        scaled = (centered * lax.rsqrt(variance + EPSILON)).T
        tri_normed = (scaled * out_gain_ref[...] + out_bias_ref[...]).astype(jnp.bfloat16)
        mixed = jnp.dot(tri_normed, out_weight_ref[...], preferred_element_type=jnp.float32)
        out_ref[q * per_tile : (q + 1) * per_tile] = (
            (gating_ref[lanes, :] * mixed).astype(jnp.bfloat16).reshape(per_tile, width, channels)
        )

    departed(right_out, right_send.at[0], plane - 1)
    departed(right_out, right_send.at[1], plane)
    departed(left_out, left_send.at[1], plane)

    @pl.when(holds_left)
    def _():
        departed(left_out, left_send.at[0], plane - 1)

    @pl.when(jnp.logical_not(holds_left))
    def _():
        departed(left_out, left_send.at[0], plane)

    @pl.when(sums_here)
    def _():
        departed(tri_in, tri_send, plane - 1)

    @pl.when(jnp.logical_not(sums_here))
    def _():
        departed(tri_in, tri_send, plane)


def fused(nx, ny, nz, *arguments):
    pair, pair_mask, in_gain, in_bias, proj_weight, gate_weight, out_gain, out_bias, out_weight = arguments
    rows, width, channels = pair.shape
    hidden = proj_weight.shape[1] // 4
    plane = ny * nz
    block = hidden // plane
    tiles = rows * width // LANES
    half = nx // 2
    owners = half * rows // width
    cut = block // CUTS
    travelling = (plane, tiles, cut, LANES)
    dma = pltpu.SemaphoreType.DMA
    return pl.pallas_call(
        functools.partial(kernel, nx, ny, nz),
        out_shape=pltpu.VMEM(pair.shape, jnp.bfloat16),
        in_specs=[pl.BlockSpec(memory_space=pltpu.HBM)] * 9,
        out_specs=pl.BlockSpec(memory_space=pltpu.VMEM),
        scratch_shapes=[
            pltpu.VMEM((CUTS, *travelling), jnp.bfloat16),
            pltpu.VMEM((CUTS, *travelling), jnp.bfloat16),
            pltpu.VMEM((CUTS, half, owners, *travelling[1:]), jnp.bfloat16),
            pltpu.VMEM((half, CUTS, *travelling), jnp.bfloat16),
            pltpu.VMEM((half, CUTS, *travelling), jnp.bfloat16),
            pltpu.VMEM((CUTS, *travelling), jnp.bfloat16),
            pltpu.VMEM((half, cut, rows, LANES), jnp.bfloat16),
            pltpu.VMEM((half, cut, rows, LANES), jnp.bfloat16),
            pltpu.VMEM((2 * half, cut * (rows + PAD), LANES), jnp.float32),
            pltpu.VMEM((half, rows * (cut + PAD), LANES), jnp.float32),
            pltpu.VMEM((rows * width, channels), jnp.bfloat16),
            pltpu.VMEM((rows * width, channels), jnp.float32),
            dma((2,)),
            dma((half, CUTS)),
            dma((2,)),
            dma((half, CUTS)),
            dma,
            dma((CUTS,)),
            pltpu.SemaphoreType.REGULAR,
            pltpu.VMEM(pair.shape, pair.dtype),
            pltpu.VMEM((width, rows), pair_mask.dtype),
            pltpu.VMEM((1, in_gain.size), in_gain.dtype),
            pltpu.VMEM((1, in_bias.size), in_bias.dtype),
            pltpu.VMEM(proj_weight.shape, proj_weight.dtype),
            pltpu.VMEM(gate_weight.shape, gate_weight.dtype),
            pltpu.VMEM((1, out_gain.size), out_gain.dtype),
            pltpu.VMEM((1, out_bias.size), out_bias.dtype),
            pltpu.VMEM(out_weight.shape, out_weight.dtype),
            dma((9,)),
        ],
        compiler_params=pltpu.CompilerParams(collective_id=0, has_side_effects=True),
    )(
        pair,
        pair_mask.T,
        in_gain.reshape(1, -1),
        in_bias.reshape(1, -1),
        proj_weight,
        gate_weight,
        out_gain.reshape(1, -1),
        out_bias.reshape(1, -1),
        out_weight,
    )


def solution(mesh):
    nx, ny, nz = mesh.shape["gx"], mesh.shape["gy"], mesh.shape["gz"]
    plane = ny * nz

    def on_device(pair, *others):
        rows, width, channels = pair.shape
        hidden = others[3].shape[1] // 4
        fits = (
            width * plane == LANES
            and rows * nx == LANES
            and rows % width == 0
            and rows * width % LANES == 0
            and nx == 4
            and channels % LANES == 0
            and hidden % (8 * CUTS * plane) == 0
        )
        if fits:
            return fused(nx, ny, nz, pair, *others)
        return with_collectives(pair, *others)

    return jax.shard_map(
        on_device,
        mesh=mesh,
        in_specs=(
            P("gx", ("gy", "gz"), None),
            P("gx", ("gy", "gz")),
            P(),
            P(),
            P(),
            P(),
            P(),
            P(),
            P(),
        ),
        out_specs=P("gx", ("gy", "gz"), None),
        check_vma=False,
    )
```

```python
import functools

import jax
import jax.numpy as jnp
from jax import lax
from jax.experimental import pallas as pl
from jax.experimental.pallas import tpu as pltpu
from jax.sharding import PartitionSpec as P

MESH = pl.DeviceIdType.MESH
LANES = 128
EPSILON = 1e-05
CUTS = 2
PAD = 1


def normalize(values, gain, bias):
    average = jnp.mean(values, axis=-1, keepdims=True)
    centered = values - average
    variance = jnp.mean(centered * centered, axis=-1, keepdims=True)
    return centered * lax.rsqrt(variance + EPSILON) * gain + bias


def project(tile, mask_value, in_gain, in_bias, proj_weight):
    hidden = proj_weight.shape[1] // 4
    normed = normalize(tile.astype(jnp.float32), in_gain, in_bias).astype(jnp.bfloat16)
    projected = jnp.einsum("rwc,cd->rwd", normed, proj_weight, preferred_element_type=jnp.float32)
    left_side = (
        jax.nn.sigmoid(projected[:, :, :hidden]) * projected[:, :, hidden : 2 * hidden] * mask_value
    ).astype(jnp.bfloat16)
    right_side = (
        jax.nn.sigmoid(projected[:, :, 2 * hidden : 3 * hidden])
        * projected[:, :, 3 * hidden :]
        * mask_value
    ).astype(jnp.bfloat16)
    return (normed, left_side, right_side)


def with_collectives(
    pair, pair_mask, in_gain, in_bias, proj_weight, gate_weight, out_gain, out_bias, out_weight
):
    mask_value = pair_mask.astype(jnp.float32)[:, :, None]
    normed, left_side, own_right = project(pair, mask_value, in_gain, in_bias, proj_weight)
    left_slab, right_slab = (
        lax.all_gather(left_side, "gy", axis=1, tiled=True),
        lax.all_gather(own_right, "gy", axis=1, tiled=True),
    )
    every_row = lax.all_gather(own_right, "gx", axis=0, tiled=True)
    row_panel = lax.all_to_all(every_row, "gy", split_axis=0, concat_axis=1, tiled=True)
    summed = lax.psum_scatter(
        jnp.einsum("jkc,ikc->jic", row_panel, left_slab, preferred_element_type=jnp.float32),
        "gz",
        scatter_dimension=0,
        tiled=True,
    )
    triangle = jnp.transpose(summed, (1, 0, 2))
    tri_normed = normalize(triangle, out_gain, out_bias).astype(jnp.bfloat16)
    gating = jax.nn.sigmoid(
        jnp.einsum("rwc,cd->rwd", normed, gate_weight, preferred_element_type=jnp.float32)
    )
    mixed = jnp.einsum("rwh,hc->rwc", tri_normed, out_weight, preferred_element_type=jnp.float32)
    return (gating * mixed).astype(jnp.bfloat16)


def swap_groups(tiles, width):
    tiles = list(tiles)
    group = lax.broadcasted_iota(jnp.int32, tiles[0].shape, 1) // width
    bit = 1
    while bit < len(tiles):
        upper = (group // bit) % 2 == 1
        for a in range(len(tiles)):
            if (a // bit) % 2 == 0:
                low, high = tiles[a], tiles[a + bit]
                tiles[a] = jnp.where(upper, pltpu.roll(high, bit * width, 1), low)
                tiles[a + bit] = jnp.where(upper, high, pltpu.roll(low, LANES - bit * width, 1))
        bit *= 2
    return tiles


def kernel(
    nx,
    ny,
    nz,
    pair_hbm,
    mask_hbm,
    in_gain_hbm,
    in_bias_hbm,
    proj_hbm,
    gate_hbm,
    out_gain_hbm,
    out_bias_hbm,
    out_weight_hbm,
    out_ref,
    right_out,
    left_out,
    tri_out,
    right_in,
    left_in,
    tri_in,
    right_all,
    left_all,
    spread,
    sums_at,
    normed_ref,
    gating_ref,
    right_send,
    right_recv,
    left_send,
    left_recv,
    tri_send,
    tri_recv,
    above_in,
    pair_ref,
    mask_ref,
    in_gain_ref,
    in_bias_ref,
    proj_ref,
    gate_ref,
    out_gain_ref,
    out_bias_ref,
    out_weight_ref,
    load_sems,
):
    rows, width, channels = pair_ref.shape
    hidden = proj_ref.shape[1] // 4
    plane = ny * nz
    block = hidden // plane
    tiles = rows * width // LANES
    per_tile = rows // tiles
    cut = block // CUTS
    part = hidden // CUTS
    half = nx // 2
    owners = half * rows // width
    x, y, z = lax.axis_index("gx"), lax.axis_index("gy"), lax.axis_index("gz")
    me = y * nz + z
    last = nx - 1
    is_inner = jnp.logical_or(x == half - 1, x == half)
    beside = x + 1 - 2 * lax.rem(x, 2)
    across = jnp.where(x < half, half, half - 1)
    near = jnp.where(is_inner, beside, x)
    slot = lax.rem(x, 2)
    slot_beside = lax.rem(beside, 2)
    first = lax.rem(x, 2) * half
    owner0 = (x // half) * owners
    holds_left = near == x
    sums_here = (me // owners) * half + x // half == x

    def at(row, d):
        return (row, d // nz, lax.rem(d, nz))

    def turn(t):
        return lax.rem(me + t, plane)

    barrier = pltpu.get_barrier_semaphore()

    def greet(row, start):
        for t in range(start, plane):
            pl.semaphore_signal(barrier, inc=1, device_id=at(row, turn(t)), device_id_type=MESH)

    @pl.when(x < half)
    def _():
        greet(x + 1, 0)

    @pl.when(jnp.logical_or(x == half, x == 1))
    def _():
        greet(x - 1, 0)

    @pl.when(is_inner)
    def _():
        greet(last, 0)

    greet(x, 1)

    arguments = (
        (pair_hbm, pair_ref),
        (mask_hbm, mask_ref),
        (in_gain_hbm, in_gain_ref),
        (in_bias_hbm, in_bias_ref),
        (proj_hbm, proj_ref),
        (gate_hbm, gate_ref),
        (out_gain_hbm, out_gain_ref),
        (out_bias_hbm, out_bias_ref),
        (out_weight_hbm, out_weight_ref),
    )
    loads = [
        pltpu.make_async_copy(held, wanted, load_sems.at[index])
        for index, (held, wanted) in enumerate(arguments)
    ]
    for load in loads:
        load.start()
    for load in (loads[0], loads[2], loads[3]):
        load.wait()

    normed_ref[...] = normalize(
        pair_ref[...].reshape(-1, channels).astype(jnp.float32), in_gain_ref[...], in_bias_ref[...]
    ).astype(jnp.bfloat16)
    loads[1].wait()
    row_of = lax.broadcasted_iota(jnp.int32, (rows, rows * width), 1) // width
    choose = (row_of == lax.broadcasted_iota(jnp.int32, row_of.shape, 0)).astype(jnp.bfloat16)
    repeated = jnp.dot(
        mask_ref[...].astype(jnp.float32).astype(jnp.bfloat16), choose, preferred_element_type=jnp.float32
    )
    column_of = lax.broadcasted_iota(jnp.int32, repeated.shape, 1) % width
    own_column = column_of == lax.broadcasted_iota(jnp.int32, repeated.shape, 0)
    mask_row = jnp.sum(jnp.where(own_column, repeated, 0.0), axis=0, keepdims=True)

    def side(base, target, h):
        gates = proj_ref[:, base + h * part : base + (h + 1) * part]
        values = proj_ref[:, base + hidden + h * part : base + hidden + (h + 1) * part]
        weight = jnp.concatenate([gates, values], axis=1).T
        for q in range(tiles):
            lanes = slice(q * LANES, (q + 1) * LANES)
            projected = lax.dot_general(
                weight, normed_ref[lanes, :], (((1,), (1,)), ((), ())), preferred_element_type=jnp.float32
            )
            value = jax.nn.sigmoid(projected[:part]) * projected[part:] * mask_row[:, lanes]
            target[h, :, q] = value.astype(jnp.bfloat16).reshape(plane, cut, LANES)

    def right_copy(far, h, t):
        d = turn(t)
        return pltpu.make_async_remote_copy(
            src_ref=right_out.at[h, d],
            dst_ref=right_in.at[slot, h, me],
            send_sem=right_send.at[far],
            recv_sem=right_recv.at[slot, h],
            device_id=at(beside if far else x, d),
            device_id_type=MESH,
        )

    def left_copy(far, h, t):
        d = turn(t)
        return pltpu.make_async_remote_copy(
            src_ref=left_out.at[h, d],
            dst_ref=left_in.at[slot, h, me],
            send_sem=left_send.at[far],
            recv_sem=left_recv.at[slot, h],
            device_id=at(across if far else near, d),
            device_id_type=MESH,
        )

    def arrived(target, sem, number):
        whole = target.at[pl.ds(0, number)]
        pltpu.make_async_remote_copy(
            src_ref=whole,
            dst_ref=whole,
            send_sem=tri_send,
            recv_sem=sem,
            device_id=at(beside, me),
            device_id_type=MESH,
        ).wait_recv()

    def departed(held, sem, number):
        whole = held.at[:, pl.ds(0, number)]
        pltpu.make_async_remote_copy(
            src_ref=whole,
            dst_ref=whole,
            send_sem=sem,
            recv_sem=tri_recv.at[0],
            device_id=at(beside, me),
            device_id_type=MESH,
        ).wait_send()

    def send_right(far, h):
        for t in range(0 if far else 1, plane):
            right_copy(far, h, t).start()

    def send_left(far, h):
        for t in range(1, plane):
            left_copy(far, h, t).start()
        if far:
            left_copy(far, h, 0).start()
        else:

            @pl.when(jnp.logical_not(holds_left))
            def _():
                left_copy(far, h, 0).start()

    def all_greeted():
        others = jnp.where(lax.rem(x, 2) == 0, 1, 2)
        pl.semaphore_wait(barrier, plane - 1 + plane * others)

    def tell():
        pl.semaphore_signal(above_in, inc=1, device_id=at(x - 1, me), device_id_type=MESH)

    def told():
        pl.semaphore_wait(above_in, 1)

    loads[4].wait()
    side(2 * hidden, right_out, 0)

    @pl.when(x == last)
    def _():
        all_greeted()
        tell()
        send_right(1, 0)

    side(0, left_out, 0)

    @pl.when(x == 0)
    def _():
        all_greeted()
        send_right(0, 0)
        send_left(0, 0)
        send_right(1, 0)

    @pl.when(x == half - 1)
    def _():
        all_greeted()
        tell()
        send_left(0, 0)
        send_left(1, 0)
        send_right(0, 0)
        send_right(1, 0)

    @pl.when(x == half)
    def _():
        all_greeted()
        send_right(0, 0)
        send_left(1, 0)

    @pl.when(x == last)
    def _():
        send_left(1, 0)
        send_right(0, 0)
        send_left(0, 0)

    side(2 * hidden, right_out, 1)
    side(0, left_out, 1)

    @pl.when(x == 0)
    def _():
        send_right(0, 1)
        send_left(0, 1)
        told()
        send_left(1, 0)
        send_left(1, 1)
        send_right(1, 1)

    @pl.when(x == half - 1)
    def _():
        send_left(0, 1)
        send_left(1, 1)
        send_right(0, 1)
        send_right(1, 1)

    @pl.when(x == half)
    def _():
        send_right(0, 1)
        send_left(1, 1)
        told()
        send_right(1, 0)
        send_left(0, 0)
        send_right(1, 1)
        send_left(0, 1)

    @pl.when(x == last)
    def _():
        send_left(1, 1)
        send_right(1, 1)
        send_right(0, 1)
        send_left(0, 1)

    for h in range(CUTS):
        right_in[slot, h, me] = right_out[h, me]

        @pl.when(holds_left)
        def _():
            left_in[slot, h, me] = left_out[h, me]

    loads[5].wait()
    gating_ref[...] = jax.nn.sigmoid(
        jnp.dot(normed_ref[...], gate_ref[...], preferred_element_type=jnp.float32)
    )

    def gather_sums(source, target, at_rows):
        for q in range(tiles):
            swapped = swap_groups([source[a, q].astype(jnp.float32) for a in range(plane)], width)
            for a in range(per_tile):
                at_rows[pl.ds(q * per_tile + a, cut, stride=rows + PAD), :] = swapped[a]
        for c in range(cut):
            target[c] = at_rows[pl.ds(c * (rows + PAD), rows), :].astype(jnp.bfloat16)

    def left_arrived(which, h):
        local = jnp.logical_and(holds_left, which == slot)

        @pl.when(local)
        def _():
            arrived(left_in.at[which, h], left_recv.at[which, h], plane - 1)

        @pl.when(jnp.logical_not(local))
        def _():
            arrived(left_in.at[which, h], left_recv.at[which, h], plane)

    def tri_copy(which, h, index):
        return pltpu.make_async_remote_copy(
            src_ref=tri_out.at[h, which, index],
            dst_ref=tri_in.at[h, me],
            send_sem=tri_send,
            recv_sem=tri_recv.at[h],
            device_id=at(first + which, owner0 + index),
            device_id_type=MESH,
        )

    def is_mine(which, index):
        return jnp.logical_and(first + which == x, owner0 + index == me)

    lane = lax.broadcasted_iota(jnp.int32, (cut, LANES), 1)
    fewer = owners // half
    for h in range(CUTS):
        for which in range(half):
            left_arrived(which, h)
        for turned, column in enumerate((slot, slot_beside)):
            arrived(right_in.at[column, h], right_recv.at[column, h], plane - 1 if turned == 0 else plane)
            gather_sums(right_in.at[column, h], right_all.at[turned], spread.at[turned])
            if turned == 0:
                for which in range(half):
                    gather_sums(left_in.at[which, h], left_all.at[which], spread.at[half + which])
            for c in range(cut):
                triangle = lax.dot_general(
                    left_all[:, c].reshape(half * rows, LANES),
                    right_all[turned, c],
                    (((1,), (1,)), ((), ())),
                    preferred_element_type=jnp.float32,
                )
                for which in range(half):
                    sums_at[which, pl.ds(c, rows, stride=cut + PAD), :rows] = triangle[
                        which * rows : (which + 1) * rows
                    ]
            for which in range(half):
                for q in range(tiles):
                    at_row = [
                        sums_at[which, pl.ds((q * per_tile + a) * (cut + PAD), cut), :]
                        for a in range(per_tile)
                    ]
                    packed = []
                    for a in range(fewer):
                        lanes_of = at_row[a]
                        for g in range(1, per_tile // fewer):
                            moved = pltpu.roll(at_row[a + g * fewer], g * fewer * width, 1)
                            lanes_of = jnp.where(lane < g * fewer * width, lanes_of, moved)
                        packed.append(lanes_of)
                    swapped = swap_groups(packed, width)
                    for index in range(fewer):
                        tri_out[h, which, column * fewer + index, q] = swapped[index].astype(jnp.bfloat16)
            for index in (column * fewer + one for one in range(fewer)):
                for which in range(half):

                    @pl.when(jnp.logical_not(is_mine(which, index)))
                    def _():
                        tri_copy(which, h, index).start()

                    @pl.when(is_mine(which, index))
                    def _():
                        tri_in[h, me] = tri_out[h, which, index]

    for load in loads[6:]:
        load.wait()

    @pl.when(sums_here)
    def _():
        for h in range(CUTS):
            arrived(tri_in.at[h], tri_recv.at[h], plane - 1)

    @pl.when(jnp.logical_not(sums_here))
    def _():
        for h in range(CUTS):
            arrived(tri_in.at[h], tri_recv.at[h], plane)

    for q in range(tiles):
        lanes = slice(q * LANES, (q + 1) * LANES)
        sums = tri_in[:, :, q].astype(jnp.float32).reshape(hidden, LANES)
        centered = sums - jnp.mean(sums, axis=0, keepdims=True)
        variance = jnp.mean(centered * centered, axis=0, keepdims=True)
        scaled = (centered * lax.rsqrt(variance + EPSILON)).T
        tri_normed = (scaled * out_gain_ref[...] + out_bias_ref[...]).astype(jnp.bfloat16)
        mixed = jnp.dot(tri_normed, out_weight_ref[...], preferred_element_type=jnp.float32)
        out_ref[q * per_tile : (q + 1) * per_tile] = (
            (gating_ref[lanes, :] * mixed).astype(jnp.bfloat16).reshape(per_tile, width, channels)
        )

    departed(right_out, right_send.at[0], plane - 1)
    departed(right_out, right_send.at[1], plane)
    departed(left_out, left_send.at[1], plane)

    @pl.when(holds_left)
    def _():
        departed(left_out, left_send.at[0], plane - 1)

    @pl.when(jnp.logical_not(holds_left))
    def _():
        departed(left_out, left_send.at[0], plane)

    @pl.when(sums_here)
    def _():
        departed(tri_in, tri_send, plane - 1)

    @pl.when(jnp.logical_not(sums_here))
    def _():
        departed(tri_in, tri_send, plane)


def fused(nx, ny, nz, *arguments):
    pair, pair_mask, in_gain, in_bias, proj_weight, gate_weight, out_gain, out_bias, out_weight = arguments
    rows, width, channels = pair.shape
    hidden = proj_weight.shape[1] // 4
    plane = ny * nz
    block = hidden // plane
    tiles = rows * width // LANES
    half = nx // 2
    owners = half * rows // width
    cut = block // CUTS
    travelling = (plane, tiles, cut, LANES)
    dma = pltpu.SemaphoreType.DMA
    return pl.pallas_call(
        functools.partial(kernel, nx, ny, nz),
        out_shape=pltpu.VMEM(pair.shape, jnp.bfloat16),
        in_specs=[pl.BlockSpec(memory_space=pltpu.HBM)] * 9,
        out_specs=pl.BlockSpec(memory_space=pltpu.VMEM),
        scratch_shapes=[
            pltpu.VMEM((CUTS, *travelling), jnp.bfloat16),
            pltpu.VMEM((CUTS, *travelling), jnp.bfloat16),
            pltpu.VMEM((CUTS, half, owners, *travelling[1:]), jnp.bfloat16),
            pltpu.VMEM((half, CUTS, *travelling), jnp.bfloat16),
            pltpu.VMEM((half, CUTS, *travelling), jnp.bfloat16),
            pltpu.VMEM((CUTS, *travelling), jnp.bfloat16),
            pltpu.VMEM((half, cut, rows, LANES), jnp.bfloat16),
            pltpu.VMEM((half, cut, rows, LANES), jnp.bfloat16),
            pltpu.VMEM((2 * half, cut * (rows + PAD), LANES), jnp.float32),
            pltpu.VMEM((half, rows * (cut + PAD), LANES), jnp.float32),
            pltpu.VMEM((rows * width, channels), jnp.bfloat16),
            pltpu.VMEM((rows * width, channels), jnp.float32),
            dma((2,)),
            dma((half, CUTS)),
            dma((2,)),
            dma((half, CUTS)),
            dma,
            dma((CUTS,)),
            pltpu.SemaphoreType.REGULAR,
            pltpu.VMEM(pair.shape, pair.dtype),
            pltpu.VMEM((width, rows), pair_mask.dtype),
            pltpu.VMEM((1, in_gain.size), in_gain.dtype),
            pltpu.VMEM((1, in_bias.size), in_bias.dtype),
            pltpu.VMEM(proj_weight.shape, proj_weight.dtype),
            pltpu.VMEM(gate_weight.shape, gate_weight.dtype),
            pltpu.VMEM((1, out_gain.size), out_gain.dtype),
            pltpu.VMEM((1, out_bias.size), out_bias.dtype),
            pltpu.VMEM(out_weight.shape, out_weight.dtype),
            dma((9,)),
        ],
        compiler_params=pltpu.CompilerParams(collective_id=0, has_side_effects=True),
    )(
        pair,
        pair_mask.T,
        in_gain.reshape(1, -1),
        in_bias.reshape(1, -1),
        proj_weight,
        gate_weight,
        out_gain.reshape(1, -1),
        out_bias.reshape(1, -1),
        out_weight,
    )


def solution(mesh):
    nx, ny, nz = mesh.shape["gx"], mesh.shape["gy"], mesh.shape["gz"]
    plane = ny * nz

    def on_device(pair, *others):
        rows, width, channels = pair.shape
        hidden = others[3].shape[1] // 4
        fits = (
            width * plane == LANES
            and rows * nx == LANES
            and rows % width == 0
            and rows * width % LANES == 0
            and nx == 4
            and channels % LANES == 0
            and hidden % (8 * CUTS * plane) == 0
        )
        if fits:
            return fused(nx, ny, nz, pair, *others)
        return with_collectives(pair, *others)

    return jax.shard_map(
        on_device,
        mesh=mesh,
        in_specs=(
            P("gx", ("gy", "gz"), None),
            P("gx", ("gy", "gz")),
            P(),
            P(),
            P(),
            P(),
            P(),
            P(),
            P(),
        ),
        out_specs=P("gx", ("gy", "gz"), None),
        check_vma=False,
    )
```

```python
import functools

import jax
import jax.numpy as jnp
from jax import lax
from jax.experimental import pallas as pl
from jax.experimental.pallas import tpu as pltpu
from jax.sharding import PartitionSpec as P

MESH = pl.DeviceIdType.MESH
LANES = 128
EPSILON = 1e-05
CUTS = 2
PAD = 1


def normalize(values, gain, bias):
    average = jnp.mean(values, axis=-1, keepdims=True)
    centered = values - average
    variance = jnp.mean(centered * centered, axis=-1, keepdims=True)
    return centered * lax.rsqrt(variance + EPSILON) * gain + bias


def project(tile, mask_value, in_gain, in_bias, proj_weight):
    hidden = proj_weight.shape[1] // 4
    normed = normalize(tile.astype(jnp.float32), in_gain, in_bias).astype(jnp.bfloat16)
    projected = jnp.einsum("rwc,cd->rwd", normed, proj_weight, preferred_element_type=jnp.float32)
    left_side = (
        jax.nn.sigmoid(projected[:, :, :hidden]) * projected[:, :, hidden : 2 * hidden] * mask_value
    ).astype(jnp.bfloat16)
    right_side = (
        jax.nn.sigmoid(projected[:, :, 2 * hidden : 3 * hidden])
        * projected[:, :, 3 * hidden :]
        * mask_value
    ).astype(jnp.bfloat16)
    return (normed, left_side, right_side)


def with_collectives(
    pair, pair_mask, in_gain, in_bias, proj_weight, gate_weight, out_gain, out_bias, out_weight
):
    mask_value = pair_mask.astype(jnp.float32)[:, :, None]
    normed, left_side, own_right = project(pair, mask_value, in_gain, in_bias, proj_weight)
    left_slab, right_slab = (
        lax.all_gather(left_side, "gy", axis=1, tiled=True),
        lax.all_gather(own_right, "gy", axis=1, tiled=True),
    )
    every_row = lax.all_gather(own_right, "gx", axis=0, tiled=True)
    row_panel = lax.all_to_all(every_row, "gy", split_axis=0, concat_axis=1, tiled=True)
    summed = lax.psum_scatter(
        jnp.einsum("jkc,ikc->jic", row_panel, left_slab, preferred_element_type=jnp.float32),
        "gz",
        scatter_dimension=0,
        tiled=True,
    )
    triangle = jnp.transpose(summed, (1, 0, 2))
    tri_normed = normalize(triangle, out_gain, out_bias).astype(jnp.bfloat16)
    gating = jax.nn.sigmoid(
        jnp.einsum("rwc,cd->rwd", normed, gate_weight, preferred_element_type=jnp.float32)
    )
    mixed = jnp.einsum("rwh,hc->rwc", tri_normed, out_weight, preferred_element_type=jnp.float32)
    return (gating * mixed).astype(jnp.bfloat16)


def swap_groups(tiles, width):
    tiles = list(tiles)
    group = lax.broadcasted_iota(jnp.int32, tiles[0].shape, 1) // width
    bit = 1
    while bit < len(tiles):
        upper = (group // bit) % 2 == 1
        for a in range(len(tiles)):
            if (a // bit) % 2 == 0:
                low, high = tiles[a], tiles[a + bit]
                tiles[a] = jnp.where(upper, pltpu.roll(high, bit * width, 1), low)
                tiles[a + bit] = jnp.where(upper, high, pltpu.roll(low, LANES - bit * width, 1))
        bit *= 2
    return tiles


def kernel(
    nx,
    ny,
    nz,
    pair_hbm,
    mask_hbm,
    in_gain_hbm,
    in_bias_hbm,
    proj_hbm,
    gate_hbm,
    out_gain_hbm,
    out_bias_hbm,
    out_weight_hbm,
    out_ref,
    right_out,
    left_out,
    tri_out,
    right_in,
    left_in,
    tri_in,
    right_all,
    left_all,
    spread,
    sums_at,
    normed_ref,
    gating_ref,
    right_send,
    right_recv,
    left_send,
    left_recv,
    tri_send,
    tri_recv,
    above_in,
    pair_ref,
    mask_ref,
    in_gain_ref,
    in_bias_ref,
    proj_ref,
    gate_ref,
    out_gain_ref,
    out_bias_ref,
    out_weight_ref,
    load_sems,
):
    rows, width, channels = pair_ref.shape
    hidden = proj_ref.shape[1] // 4
    plane = ny * nz
    block = hidden // plane
    tiles = rows * width // LANES
    per_tile = rows // tiles
    cut = block // CUTS
    part = hidden // CUTS
    half = nx // 2
    owners = half * rows // width
    x, y, z = lax.axis_index("gx"), lax.axis_index("gy"), lax.axis_index("gz")
    me = y * nz + z
    last = nx - 1
    is_inner = jnp.logical_or(x == half - 1, x == half)
    beside = x + 1 - 2 * lax.rem(x, 2)
    across = jnp.where(x < half, half, half - 1)
    near = jnp.where(is_inner, beside, x)
    slot = lax.rem(x, 2)
    slot_beside = lax.rem(beside, 2)
    first = lax.rem(x, 2) * half
    owner0 = (x // half) * owners
    holds_left = near == x
    sums_here = (me // owners) * half + x // half == x

    def at(row, d):
        return (row, d // nz, lax.rem(d, nz))

    def turn(t):
        return lax.rem(me + t, plane)

    barrier = pltpu.get_barrier_semaphore()

    def greet(row, start):
        for t in range(start, plane):
            pl.semaphore_signal(barrier, inc=1, device_id=at(row, turn(t)), device_id_type=MESH)

    @pl.when(x < half)
    def _():
        greet(x + 1, 0)

    @pl.when(jnp.logical_or(x == half, x == 1))
    def _():
        greet(x - 1, 0)

    @pl.when(is_inner)
    def _():
        greet(last, 0)

    greet(x, 1)

    arguments = (
        (pair_hbm, pair_ref),
        (mask_hbm, mask_ref),
        (in_gain_hbm, in_gain_ref),
        (in_bias_hbm, in_bias_ref),
        (proj_hbm, proj_ref),
        (gate_hbm, gate_ref),
        (out_gain_hbm, out_gain_ref),
        (out_bias_hbm, out_bias_ref),
        (out_weight_hbm, out_weight_ref),
    )
    loads = [
        pltpu.make_async_copy(held, wanted, load_sems.at[index])
        for index, (held, wanted) in enumerate(arguments)
    ]
    for load in loads:
        load.start()
    for load in (loads[0], loads[2], loads[3]):
        load.wait()

    normed_ref[...] = normalize(
        pair_ref[...].reshape(-1, channels).astype(jnp.float32), in_gain_ref[...], in_bias_ref[...]
    ).astype(jnp.bfloat16)
    loads[1].wait()
    row_of = lax.broadcasted_iota(jnp.int32, (rows, rows * width), 1) // width
    choose = (row_of == lax.broadcasted_iota(jnp.int32, row_of.shape, 0)).astype(jnp.bfloat16)
    repeated = jnp.dot(
        mask_ref[...].astype(jnp.float32).astype(jnp.bfloat16), choose, preferred_element_type=jnp.float32
    )
    column_of = lax.broadcasted_iota(jnp.int32, repeated.shape, 1) % width
    own_column = column_of == lax.broadcasted_iota(jnp.int32, repeated.shape, 0)
    mask_row = jnp.sum(jnp.where(own_column, repeated, 0.0), axis=0, keepdims=True)

    def side(base, target, h):
        gates = proj_ref[:, base + h * part : base + (h + 1) * part]
        values = proj_ref[:, base + hidden + h * part : base + hidden + (h + 1) * part]
        weight = jnp.concatenate([gates, values], axis=1).T
        for q in range(tiles):
            lanes = slice(q * LANES, (q + 1) * LANES)
            projected = lax.dot_general(
                weight, normed_ref[lanes, :], (((1,), (1,)), ((), ())), preferred_element_type=jnp.float32
            )
            value = jax.nn.sigmoid(projected[:part]) * projected[part:] * mask_row[:, lanes]
            target[h, :, q] = value.astype(jnp.bfloat16).reshape(plane, cut, LANES)

    def right_copy(far, h, t):
        d = turn(t)
        return pltpu.make_async_remote_copy(
            src_ref=right_out.at[h, d],
            dst_ref=right_in.at[slot, h, me],
            send_sem=right_send.at[far],
            recv_sem=right_recv.at[slot, h],
            device_id=at(beside if far else x, d),
            device_id_type=MESH,
        )

    def left_copy(far, h, t):
        d = turn(t)
        return pltpu.make_async_remote_copy(
            src_ref=left_out.at[h, d],
            dst_ref=left_in.at[slot, h, me],
            send_sem=left_send.at[far],
            recv_sem=left_recv.at[slot, h],
            device_id=at(across if far else near, d),
            device_id_type=MESH,
        )

    def arrived(target, sem, number):
        whole = target.at[pl.ds(0, number)]
        pltpu.make_async_remote_copy(
            src_ref=whole,
            dst_ref=whole,
            send_sem=tri_send,
            recv_sem=sem,
            device_id=at(beside, me),
            device_id_type=MESH,
        ).wait_recv()

    def departed(held, sem, number):
        whole = held.at[:, pl.ds(0, number)]
        pltpu.make_async_remote_copy(
            src_ref=whole,
            dst_ref=whole,
            send_sem=sem,
            recv_sem=tri_recv.at[0],
            device_id=at(beside, me),
            device_id_type=MESH,
        ).wait_send()

    def send_right(far, h):
        for t in range(0 if far else 1, plane):
            right_copy(far, h, t).start()

    def send_left(far, h):
        for t in range(1, plane):
            left_copy(far, h, t).start()
        if far:
            left_copy(far, h, 0).start()
        else:

            @pl.when(jnp.logical_not(holds_left))
            def _():
                left_copy(far, h, 0).start()

    def all_greeted():
        others = jnp.where(lax.rem(x, 2) == 0, 1, 2)
        pl.semaphore_wait(barrier, plane - 1 + plane * others)

    def tell():
        pl.semaphore_signal(above_in, inc=1, device_id=at(x - 1, me), device_id_type=MESH)

    def told():
        pl.semaphore_wait(above_in, 1)

    loads[4].wait()
    side(2 * hidden, right_out, 0)

    @pl.when(x == last)
    def _():
        all_greeted()
        tell()
        send_right(1, 0)

    side(0, left_out, 0)

    @pl.when(x == 0)
    def _():
        all_greeted()
        send_right(1, 0)
        send_right(0, 0)
        send_left(0, 0)

    @pl.when(x == half - 1)
    def _():
        all_greeted()
        tell()
        send_left(1, 0)
        send_left(0, 0)
        send_right(0, 0)

    @pl.when(x == half)
    def _():
        all_greeted()
        send_right(0, 0)
        send_left(1, 0)

    @pl.when(x == last)
    def _():
        send_left(1, 0)
        send_right(0, 0)
        send_left(0, 0)

    side(2 * hidden, right_out, 1)
    side(0, left_out, 1)

    @pl.when(x == 0)
    def _():
        told()
        send_left(1, 0)
        send_left(1, 1)
        send_right(0, 1)
        send_left(0, 1)
        send_right(1, 1)

    @pl.when(x == half - 1)
    def _():
        send_left(1, 1)
        send_left(0, 1)
        send_right(1, 0)
        send_right(0, 1)
        send_right(1, 1)

    @pl.when(x == half)
    def _():
        send_right(0, 1)
        send_left(1, 1)
        told()
        send_right(1, 0)
        send_left(0, 0)
        send_right(1, 1)
        send_left(0, 1)

    @pl.when(x == last)
    def _():
        send_left(1, 1)
        send_right(1, 1)
        send_right(0, 1)
        send_left(0, 1)

    for h in range(CUTS):
        right_in[slot, h, me] = right_out[h, me]

        @pl.when(holds_left)
        def _():
            left_in[slot, h, me] = left_out[h, me]

    loads[5].wait()
    gating_ref[...] = jax.nn.sigmoid(
        jnp.dot(normed_ref[...], gate_ref[...], preferred_element_type=jnp.float32)
    )

    def gather_sums(source, target, at_rows):
        for q in range(tiles):
            swapped = swap_groups([source[a, q].astype(jnp.float32) for a in range(plane)], width)
            for a in range(per_tile):
                at_rows[pl.ds(q * per_tile + a, cut, stride=rows + PAD), :] = swapped[a]
        for c in range(cut):
            target[c] = at_rows[pl.ds(c * (rows + PAD), rows), :].astype(jnp.bfloat16)

    def left_arrived(which, h):
        local = jnp.logical_and(holds_left, which == slot)

        @pl.when(local)
        def _():
            arrived(left_in.at[which, h], left_recv.at[which, h], plane - 1)

        @pl.when(jnp.logical_not(local))
        def _():
            arrived(left_in.at[which, h], left_recv.at[which, h], plane)

    def tri_copy(which, h, index):
        return pltpu.make_async_remote_copy(
            src_ref=tri_out.at[h, which, index],
            dst_ref=tri_in.at[h, me],
            send_sem=tri_send,
            recv_sem=tri_recv.at[h],
            device_id=at(first + which, owner0 + index),
            device_id_type=MESH,
        )

    def is_mine(which, index):
        return jnp.logical_and(first + which == x, owner0 + index == me)

    lane = lax.broadcasted_iota(jnp.int32, (cut, LANES), 1)
    fewer = owners // half

    def sums_of(turned, h):
        column = slot_beside if turned else slot
        if turned == 0:
            for which in range(half):
                left_arrived(which, h)
        arrived(right_in.at[column, h], right_recv.at[column, h], plane - 1 if turned == 0 else plane)
        gather_sums(right_in.at[column, h], right_all.at[turned], spread.at[turned])
        if turned == 0:
            for which in range(half):
                gather_sums(left_in.at[which, h], left_all.at[h, which], spread.at[half + which])
        for c in range(cut):
            triangle = lax.dot_general(
                left_all[h, :, c].reshape(half * rows, LANES),
                right_all[turned, c],
                (((1,), (1,)), ((), ())),
                preferred_element_type=jnp.float32,
            )
            for which in range(half):
                sums_at[which, pl.ds(c, rows, stride=cut + PAD), :rows] = triangle[
                    which * rows : (which + 1) * rows
                ]
        for which in range(half):
            for q in range(tiles):
                at_row = [
                    sums_at[which, pl.ds((q * per_tile + a) * (cut + PAD), cut), :]
                    for a in range(per_tile)
                ]
                packed = []
                for a in range(fewer):
                    lanes_of = at_row[a]
                    for g in range(1, per_tile // fewer):
                        moved = pltpu.roll(at_row[a + g * fewer], g * fewer * width, 1)
                        lanes_of = jnp.where(lane < g * fewer * width, lanes_of, moved)
                    packed.append(lanes_of)
                swapped = swap_groups(packed, width)
                for index in range(fewer):
                    tri_out[h, which, column * fewer + index, q] = swapped[index].astype(jnp.bfloat16)
        for index in (column * fewer + one for one in reversed(range(fewer))):
            for which in range(half):

                @pl.when(jnp.logical_not(is_mine(which, index)))
                def _():
                    tri_copy(which, h, index).start()

                @pl.when(is_mine(which, index))
                def _():
                    tri_in[h, me] = tri_out[h, which, index]

    sums_of(0, 0)

    @pl.when(x == 0)
    def _():
        sums_of(0, 1)

    sums_of(1, 0)

    @pl.when(x != 0)
    def _():
        sums_of(0, 1)

    sums_of(1, 1)

    for load in loads[6:]:
        load.wait()

    @pl.when(sums_here)
    def _():
        for h in range(CUTS):
            arrived(tri_in.at[h], tri_recv.at[h], plane - 1)

    @pl.when(jnp.logical_not(sums_here))
    def _():
        for h in range(CUTS):
            arrived(tri_in.at[h], tri_recv.at[h], plane)

    for q in range(tiles):
        lanes = slice(q * LANES, (q + 1) * LANES)
        sums = tri_in[:, :, q].astype(jnp.float32).reshape(hidden, LANES)
        centered = sums - jnp.mean(sums, axis=0, keepdims=True)
        variance = jnp.mean(centered * centered, axis=0, keepdims=True)
        scaled = (centered * lax.rsqrt(variance + EPSILON)).T
        tri_normed = (scaled * out_gain_ref[...] + out_bias_ref[...]).astype(jnp.bfloat16)
        mixed = jnp.dot(tri_normed, out_weight_ref[...], preferred_element_type=jnp.float32)
        out_ref[q * per_tile : (q + 1) * per_tile] = (
            (gating_ref[lanes, :] * mixed).astype(jnp.bfloat16).reshape(per_tile, width, channels)
        )

    departed(right_out, right_send.at[0], plane - 1)
    departed(right_out, right_send.at[1], plane)
    departed(left_out, left_send.at[1], plane)

    @pl.when(holds_left)
    def _():
        departed(left_out, left_send.at[0], plane - 1)

    @pl.when(jnp.logical_not(holds_left))
    def _():
        departed(left_out, left_send.at[0], plane)

    @pl.when(sums_here)
    def _():
        departed(tri_in, tri_send, plane - 1)

    @pl.when(jnp.logical_not(sums_here))
    def _():
        departed(tri_in, tri_send, plane)


def fused(nx, ny, nz, *arguments):
    pair, pair_mask, in_gain, in_bias, proj_weight, gate_weight, out_gain, out_bias, out_weight = arguments
    rows, width, channels = pair.shape
    hidden = proj_weight.shape[1] // 4
    plane = ny * nz
    block = hidden // plane
    tiles = rows * width // LANES
    half = nx // 2
    owners = half * rows // width
    cut = block // CUTS
    travelling = (plane, tiles, cut, LANES)
    dma = pltpu.SemaphoreType.DMA
    return pl.pallas_call(
        functools.partial(kernel, nx, ny, nz),
        out_shape=pltpu.VMEM(pair.shape, jnp.bfloat16),
        in_specs=[pl.BlockSpec(memory_space=pltpu.HBM)] * 9,
        out_specs=pl.BlockSpec(memory_space=pltpu.VMEM),
        scratch_shapes=[
            pltpu.VMEM((CUTS, *travelling), jnp.bfloat16),
            pltpu.VMEM((CUTS, *travelling), jnp.bfloat16),
            pltpu.VMEM((CUTS, half, owners, *travelling[1:]), jnp.bfloat16),
            pltpu.VMEM((half, CUTS, *travelling), jnp.bfloat16),
            pltpu.VMEM((half, CUTS, *travelling), jnp.bfloat16),
            pltpu.VMEM((CUTS, *travelling), jnp.bfloat16),
            pltpu.VMEM((half, cut, rows, LANES), jnp.bfloat16),
            pltpu.VMEM((CUTS, half, cut, rows, LANES), jnp.bfloat16),
            pltpu.VMEM((2 * half, cut * (rows + PAD), LANES), jnp.float32),
            pltpu.VMEM((half, rows * (cut + PAD), LANES), jnp.float32),
            pltpu.VMEM((rows * width, channels), jnp.bfloat16),
            pltpu.VMEM((rows * width, channels), jnp.float32),
            dma((2,)),
            dma((half, CUTS)),
            dma((2,)),
            dma((half, CUTS)),
            dma,
            dma((CUTS,)),
            pltpu.SemaphoreType.REGULAR,
            pltpu.VMEM(pair.shape, pair.dtype),
            pltpu.VMEM((width, rows), pair_mask.dtype),
            pltpu.VMEM((1, in_gain.size), in_gain.dtype),
            pltpu.VMEM((1, in_bias.size), in_bias.dtype),
            pltpu.VMEM(proj_weight.shape, proj_weight.dtype),
            pltpu.VMEM(gate_weight.shape, gate_weight.dtype),
            pltpu.VMEM((1, out_gain.size), out_gain.dtype),
            pltpu.VMEM((1, out_bias.size), out_bias.dtype),
            pltpu.VMEM(out_weight.shape, out_weight.dtype),
            dma((9,)),
        ],
        compiler_params=pltpu.CompilerParams(collective_id=0, has_side_effects=True),
    )(
        pair,
        pair_mask.T,
        in_gain.reshape(1, -1),
        in_bias.reshape(1, -1),
        proj_weight,
        gate_weight,
        out_gain.reshape(1, -1),
        out_bias.reshape(1, -1),
        out_weight,
    )


def solution(mesh):
    nx, ny, nz = mesh.shape["gx"], mesh.shape["gy"], mesh.shape["gz"]
    plane = ny * nz

    def on_device(pair, *others):
        rows, width, channels = pair.shape
        hidden = others[3].shape[1] // 4
        fits = (
            width * plane == LANES
            and rows * nx == LANES
            and rows % width == 0
            and rows * width % LANES == 0
            and nx == 4
            and channels % LANES == 0
            and hidden % (8 * CUTS * plane) == 0
        )
        if fits:
            return fused(nx, ny, nz, pair, *others)
        return with_collectives(pair, *others)

    return jax.shard_map(
        on_device,
        mesh=mesh,
        in_specs=(
            P("gx", ("gy", "gz"), None),
            P("gx", ("gy", "gz")),
            P(),
            P(),
            P(),
            P(),
            P(),
            P(),
            P(),
        ),
        out_specs=P("gx", ("gy", "gz"), None),
        check_vma=False,
    )
```

```python
import functools

import jax
import jax.numpy as jnp
from jax import lax
from jax.experimental import pallas as pl
from jax.experimental.pallas import tpu as pltpu
from jax.sharding import PartitionSpec as P

MESH = pl.DeviceIdType.MESH
LANES = 128
EPSILON = 1e-05
CUTS = 2
PAD = 1


def normalize(values, gain, bias):
    average = jnp.mean(values, axis=-1, keepdims=True)
    centered = values - average
    variance = jnp.mean(centered * centered, axis=-1, keepdims=True)
    return centered * lax.rsqrt(variance + EPSILON) * gain + bias


def project(tile, mask_value, in_gain, in_bias, proj_weight):
    hidden = proj_weight.shape[1] // 4
    normed = normalize(tile.astype(jnp.float32), in_gain, in_bias).astype(jnp.bfloat16)
    projected = jnp.einsum("rwc,cd->rwd", normed, proj_weight, preferred_element_type=jnp.float32)
    left_side = (
        jax.nn.sigmoid(projected[:, :, :hidden]) * projected[:, :, hidden : 2 * hidden] * mask_value
    ).astype(jnp.bfloat16)
    right_side = (
        jax.nn.sigmoid(projected[:, :, 2 * hidden : 3 * hidden])
        * projected[:, :, 3 * hidden :]
        * mask_value
    ).astype(jnp.bfloat16)
    return (normed, left_side, right_side)


def with_collectives(
    pair, pair_mask, in_gain, in_bias, proj_weight, gate_weight, out_gain, out_bias, out_weight
):
    mask_value = pair_mask.astype(jnp.float32)[:, :, None]
    normed, left_side, own_right = project(pair, mask_value, in_gain, in_bias, proj_weight)
    left_slab, right_slab = (
        lax.all_gather(left_side, "gy", axis=1, tiled=True),
        lax.all_gather(own_right, "gy", axis=1, tiled=True),
    )
    every_row = lax.all_gather(own_right, "gx", axis=0, tiled=True)
    row_panel = lax.all_to_all(every_row, "gy", split_axis=0, concat_axis=1, tiled=True)
    summed = lax.psum_scatter(
        jnp.einsum("jkc,ikc->jic", row_panel, left_slab, preferred_element_type=jnp.float32),
        "gz",
        scatter_dimension=0,
        tiled=True,
    )
    triangle = jnp.transpose(summed, (1, 0, 2))
    tri_normed = normalize(triangle, out_gain, out_bias).astype(jnp.bfloat16)
    gating = jax.nn.sigmoid(
        jnp.einsum("rwc,cd->rwd", normed, gate_weight, preferred_element_type=jnp.float32)
    )
    mixed = jnp.einsum("rwh,hc->rwc", tri_normed, out_weight, preferred_element_type=jnp.float32)
    return (gating * mixed).astype(jnp.bfloat16)


def swap_groups(tiles, width):
    tiles = list(tiles)
    group = lax.broadcasted_iota(jnp.int32, tiles[0].shape, 1) // width
    bit = 1
    while bit < len(tiles):
        upper = (group // bit) % 2 == 1
        for a in range(len(tiles)):
            if (a // bit) % 2 == 0:
                low, high = tiles[a], tiles[a + bit]
                tiles[a] = jnp.where(upper, pltpu.roll(high, bit * width, 1), low)
                tiles[a + bit] = jnp.where(upper, high, pltpu.roll(low, LANES - bit * width, 1))
        bit *= 2
    return tiles


def kernel(
    nx,
    ny,
    nz,
    pair_hbm,
    mask_hbm,
    in_gain_hbm,
    in_bias_hbm,
    proj_hbm,
    gate_hbm,
    out_gain_hbm,
    out_bias_hbm,
    out_weight_hbm,
    out_ref,
    right_out,
    left_out,
    tri_out,
    right_in,
    left_in,
    tri_in,
    right_all,
    left_all,
    spread,
    sums_at,
    normed_ref,
    gating_ref,
    right_send,
    right_recv,
    left_send,
    left_recv,
    tri_send,
    tri_recv,
    above_in,
    pair_ref,
    mask_ref,
    in_gain_ref,
    in_bias_ref,
    proj_ref,
    gate_ref,
    out_gain_ref,
    out_bias_ref,
    out_weight_ref,
    load_sems,
):
    rows, width, channels = pair_ref.shape
    hidden = proj_ref.shape[1] // 4
    plane = ny * nz
    block = hidden // plane
    tiles = rows * width // LANES
    per_tile = rows // tiles
    cut = block // CUTS
    part = hidden // CUTS
    half = nx // 2
    owners = half * rows // width
    x, y, z = lax.axis_index("gx"), lax.axis_index("gy"), lax.axis_index("gz")
    me = y * nz + z
    last = nx - 1
    is_inner = jnp.logical_or(x == half - 1, x == half)
    beside = x + 1 - 2 * lax.rem(x, 2)
    across = jnp.where(x < half, half, half - 1)
    near = jnp.where(is_inner, beside, x)
    slot = lax.rem(x, 2)
    slot_beside = lax.rem(beside, 2)
    first = lax.rem(x, 2) * half
    owner0 = (x // half) * owners
    holds_left = near == x
    sums_here = (me // owners) * half + x // half == x

    def at(row, d):
        return (row, d // nz, lax.rem(d, nz))

    def turn(t):
        return lax.rem(me + t, plane)

    barrier = pltpu.get_barrier_semaphore()

    def greet(row, start):
        for t in range(start, plane):
            pl.semaphore_signal(barrier, inc=1, device_id=at(row, turn(t)), device_id_type=MESH)

    @pl.when(x < half)
    def _():
        greet(x + 1, 0)

    @pl.when(jnp.logical_or(x == half, x == 1))
    def _():
        greet(x - 1, 0)

    @pl.when(is_inner)
    def _():
        greet(last, 0)

    greet(x, 1)

    arguments = (
        (pair_hbm, pair_ref),
        (mask_hbm, mask_ref),
        (in_gain_hbm, in_gain_ref),
        (in_bias_hbm, in_bias_ref),
        (proj_hbm, proj_ref),
        (gate_hbm, gate_ref),
        (out_gain_hbm, out_gain_ref),
        (out_bias_hbm, out_bias_ref),
        (out_weight_hbm, out_weight_ref),
    )
    loads = [
        pltpu.make_async_copy(held, wanted, load_sems.at[index])
        for index, (held, wanted) in enumerate(arguments)
    ]
    for load in loads:
        load.start()
    for load in (loads[0], loads[2], loads[3]):
        load.wait()

    normed_ref[...] = normalize(
        pair_ref[...].reshape(-1, channels).astype(jnp.float32), in_gain_ref[...], in_bias_ref[...]
    ).astype(jnp.bfloat16)
    loads[1].wait()
    row_of = lax.broadcasted_iota(jnp.int32, (rows, rows * width), 1) // width
    choose = (row_of == lax.broadcasted_iota(jnp.int32, row_of.shape, 0)).astype(jnp.bfloat16)
    repeated = jnp.dot(
        mask_ref[...].astype(jnp.float32).astype(jnp.bfloat16), choose, preferred_element_type=jnp.float32
    )
    column_of = lax.broadcasted_iota(jnp.int32, repeated.shape, 1) % width
    own_column = column_of == lax.broadcasted_iota(jnp.int32, repeated.shape, 0)
    mask_row = jnp.sum(jnp.where(own_column, repeated, 0.0), axis=0, keepdims=True)

    def side(base, target, h):
        gates = proj_ref[:, base + h * part : base + (h + 1) * part]
        values = proj_ref[:, base + hidden + h * part : base + hidden + (h + 1) * part]
        weight = jnp.concatenate([gates, values], axis=1).T
        for q in range(tiles):
            lanes = slice(q * LANES, (q + 1) * LANES)
            projected = lax.dot_general(
                weight, normed_ref[lanes, :], (((1,), (1,)), ((), ())), preferred_element_type=jnp.float32
            )
            value = jax.nn.sigmoid(projected[:part]) * projected[part:] * mask_row[:, lanes]
            target[h, :, q] = value.astype(jnp.bfloat16).reshape(plane, cut, LANES)

    def right_copy(far, h, t):
        d = turn(t)
        return pltpu.make_async_remote_copy(
            src_ref=right_out.at[h, d],
            dst_ref=right_in.at[slot, h, me],
            send_sem=right_send.at[far],
            recv_sem=right_recv.at[slot, h],
            device_id=at(beside if far else x, d),
            device_id_type=MESH,
        )

    def left_copy(far, h, t):
        d = turn(t)
        return pltpu.make_async_remote_copy(
            src_ref=left_out.at[h, d],
            dst_ref=left_in.at[slot, h, me],
            send_sem=left_send.at[far],
            recv_sem=left_recv.at[slot, h],
            device_id=at(across if far else near, d),
            device_id_type=MESH,
        )

    def arrived(target, sem, number):
        whole = target.at[pl.ds(0, number)]
        pltpu.make_async_remote_copy(
            src_ref=whole,
            dst_ref=whole,
            send_sem=tri_send,
            recv_sem=sem,
            device_id=at(beside, me),
            device_id_type=MESH,
        ).wait_recv()

    def departed(held, sem, number):
        whole = held.at[:, pl.ds(0, number)]
        pltpu.make_async_remote_copy(
            src_ref=whole,
            dst_ref=whole,
            send_sem=sem,
            recv_sem=tri_recv.at[0],
            device_id=at(beside, me),
            device_id_type=MESH,
        ).wait_send()

    def send_right(far, h):
        for t in range(0 if far else 1, plane):
            right_copy(far, h, t).start()

    def send_left(far, h):
        for t in range(1, plane):
            left_copy(far, h, t).start()
        if far:
            left_copy(far, h, 0).start()
        else:

            @pl.when(jnp.logical_not(holds_left))
            def _():
                left_copy(far, h, 0).start()

    def all_greeted():
        others = jnp.where(lax.rem(x, 2) == 0, 1, 2)
        pl.semaphore_wait(barrier, plane - 1 + plane * others)

    def tell():
        pl.semaphore_signal(above_in, inc=1, device_id=at(x - 1, me), device_id_type=MESH)

    def told():
        pl.semaphore_wait(above_in, 1)

    loads[4].wait()
    side(2 * hidden, right_out, 0)

    @pl.when(x == last)
    def _():
        all_greeted()
        tell()
        send_right(1, 0)

    side(0, left_out, 0)

    @pl.when(x == 0)
    def _():
        all_greeted()
        send_right(1, 0)
        send_right(0, 0)
        send_left(0, 0)

    @pl.when(x == half - 1)
    def _():
        all_greeted()
        tell()
        send_left(1, 0)
        send_left(0, 0)
        send_right(0, 0)

    @pl.when(x == half)
    def _():
        all_greeted()
        send_right(0, 0)
        send_left(1, 0)

    @pl.when(x == last)
    def _():
        send_left(1, 0)
        send_right(0, 0)
        send_left(0, 0)

    side(2 * hidden, right_out, 1)
    side(0, left_out, 1)

    @pl.when(x == 0)
    def _():
        told()
        send_left(1, 0)
        send_left(1, 1)
        send_right(0, 1)
        send_left(0, 1)
        send_right(1, 1)

    @pl.when(x == half - 1)
    def _():
        send_left(1, 1)
        send_left(0, 1)
        send_right(1, 0)
        send_right(0, 1)
        send_right(1, 1)

    @pl.when(x == half)
    def _():
        send_right(0, 1)
        send_left(1, 1)
        told()
        send_right(1, 0)
        send_left(0, 0)
        send_right(1, 1)
        send_left(0, 1)

    @pl.when(x == last)
    def _():
        send_left(1, 1)
        send_right(1, 1)
        send_right(0, 1)
        send_left(0, 1)

    for h in range(CUTS):
        right_in[slot, h, me] = right_out[h, me]

        @pl.when(holds_left)
        def _():
            left_in[slot, h, me] = left_out[h, me]

    loads[5].wait()
    gating_ref[...] = jax.nn.sigmoid(
        jnp.dot(normed_ref[...], gate_ref[...], preferred_element_type=jnp.float32)
    )

    def gather_sums(source, target, at_rows):
        for q in range(tiles):
            swapped = swap_groups([source[a, q].astype(jnp.float32) for a in range(plane)], width)
            for a in range(per_tile):
                at_rows[pl.ds(q * per_tile + a, cut, stride=rows + PAD), :] = swapped[a]
        for c in range(cut):
            target[c] = at_rows[pl.ds(c * (rows + PAD), rows), :].astype(jnp.bfloat16)

    def left_arrived(which, h):
        local = jnp.logical_and(holds_left, which == slot)

        @pl.when(local)
        def _():
            arrived(left_in.at[which, h], left_recv.at[which, h], plane - 1)

        @pl.when(jnp.logical_not(local))
        def _():
            arrived(left_in.at[which, h], left_recv.at[which, h], plane)

    def tri_copy(which, h, index):
        return pltpu.make_async_remote_copy(
            src_ref=tri_out.at[h, which, index],
            dst_ref=tri_in.at[h, me],
            send_sem=tri_send,
            recv_sem=tri_recv.at[h],
            device_id=at(first + which, owner0 + index),
            device_id_type=MESH,
        )

    def is_mine(which, index):
        return jnp.logical_and(first + which == x, owner0 + index == me)

    lane = lax.broadcasted_iota(jnp.int32, (cut, LANES), 1)
    fewer = owners // half

    def sums_of(turned, h):
        column = slot_beside if turned else slot
        if turned == 0:
            for which in range(half):
                left_arrived(which, h)
        arrived(right_in.at[column, h], right_recv.at[column, h], plane - 1 if turned == 0 else plane)
        gather_sums(right_in.at[column, h], right_all.at[turned], spread.at[turned])
        if turned == 0:
            for which in range(half):
                gather_sums(left_in.at[which, h], left_all.at[h, which], spread.at[half + which])
        for c in range(cut):
            triangle = lax.dot_general(
                left_all[h, :, c].reshape(half * rows, LANES),
                right_all[turned, c],
                (((1,), (1,)), ((), ())),
                preferred_element_type=jnp.float32,
            )
            for which in range(half):
                sums_at[which, pl.ds(c, rows, stride=cut + PAD), :rows] = triangle[
                    which * rows : (which + 1) * rows
                ]
        for which in range(half):
            for q in range(tiles):
                at_row = [
                    sums_at[which, pl.ds((q * per_tile + a) * (cut + PAD), cut), :]
                    for a in range(per_tile)
                ]
                packed = []
                for a in range(fewer):
                    lanes_of = at_row[a]
                    for g in range(1, per_tile // fewer):
                        moved = pltpu.roll(at_row[a + g * fewer], g * fewer * width, 1)
                        lanes_of = jnp.where(lane < g * fewer * width, lanes_of, moved)
                    packed.append(lanes_of)
                swapped = swap_groups(packed, width)
                for index in range(fewer):
                    tri_out[h, which, column * fewer + index, q] = swapped[index].astype(jnp.bfloat16)
        for which in range(half):
            for index in (column * fewer + one for one in reversed(range(fewer))):

                @pl.when(jnp.logical_not(is_mine(which, index)))
                def _():
                    tri_copy(which, h, index).start()

                @pl.when(is_mine(which, index))
                def _():
                    tri_in[h, me] = tri_out[h, which, index]

    sums_of(0, 0)

    @pl.when(x == 0)
    def _():
        sums_of(0, 1)

    sums_of(1, 0)

    @pl.when(x != 0)
    def _():
        sums_of(0, 1)

    sums_of(1, 1)

    for load in loads[6:]:
        load.wait()

    @pl.when(sums_here)
    def _():
        for h in range(CUTS):
            arrived(tri_in.at[h], tri_recv.at[h], plane - 1)

    @pl.when(jnp.logical_not(sums_here))
    def _():
        for h in range(CUTS):
            arrived(tri_in.at[h], tri_recv.at[h], plane)

    for q in range(tiles):
        lanes = slice(q * LANES, (q + 1) * LANES)
        sums = tri_in[:, :, q].astype(jnp.float32).reshape(hidden, LANES)
        centered = sums - jnp.mean(sums, axis=0, keepdims=True)
        variance = jnp.mean(centered * centered, axis=0, keepdims=True)
        scaled = (centered * lax.rsqrt(variance + EPSILON)).T
        tri_normed = (scaled * out_gain_ref[...] + out_bias_ref[...]).astype(jnp.bfloat16)
        mixed = jnp.dot(tri_normed, out_weight_ref[...], preferred_element_type=jnp.float32)
        out_ref[q * per_tile : (q + 1) * per_tile] = (
            (gating_ref[lanes, :] * mixed).astype(jnp.bfloat16).reshape(per_tile, width, channels)
        )

    departed(right_out, right_send.at[0], plane - 1)
    departed(right_out, right_send.at[1], plane)
    departed(left_out, left_send.at[1], plane)

    @pl.when(holds_left)
    def _():
        departed(left_out, left_send.at[0], plane - 1)

    @pl.when(jnp.logical_not(holds_left))
    def _():
        departed(left_out, left_send.at[0], plane)

    @pl.when(sums_here)
    def _():
        departed(tri_in, tri_send, plane - 1)

    @pl.when(jnp.logical_not(sums_here))
    def _():
        departed(tri_in, tri_send, plane)


def fused(nx, ny, nz, *arguments):
    pair, pair_mask, in_gain, in_bias, proj_weight, gate_weight, out_gain, out_bias, out_weight = arguments
    rows, width, channels = pair.shape
    hidden = proj_weight.shape[1] // 4
    plane = ny * nz
    block = hidden // plane
    tiles = rows * width // LANES
    half = nx // 2
    owners = half * rows // width
    cut = block // CUTS
    travelling = (plane, tiles, cut, LANES)
    dma = pltpu.SemaphoreType.DMA
    return pl.pallas_call(
        functools.partial(kernel, nx, ny, nz),
        out_shape=pltpu.VMEM(pair.shape, jnp.bfloat16),
        in_specs=[pl.BlockSpec(memory_space=pltpu.HBM)] * 9,
        out_specs=pl.BlockSpec(memory_space=pltpu.VMEM),
        scratch_shapes=[
            pltpu.VMEM((CUTS, *travelling), jnp.bfloat16),
            pltpu.VMEM((CUTS, *travelling), jnp.bfloat16),
            pltpu.VMEM((CUTS, half, owners, *travelling[1:]), jnp.bfloat16),
            pltpu.VMEM((half, CUTS, *travelling), jnp.bfloat16),
            pltpu.VMEM((half, CUTS, *travelling), jnp.bfloat16),
            pltpu.VMEM((CUTS, *travelling), jnp.bfloat16),
            pltpu.VMEM((half, cut, rows, LANES), jnp.bfloat16),
            pltpu.VMEM((CUTS, half, cut, rows, LANES), jnp.bfloat16),
            pltpu.VMEM((2 * half, cut * (rows + PAD), LANES), jnp.float32),
            pltpu.VMEM((half, rows * (cut + PAD), LANES), jnp.float32),
            pltpu.VMEM((rows * width, channels), jnp.bfloat16),
            pltpu.VMEM((rows * width, channels), jnp.float32),
            dma((2,)),
            dma((half, CUTS)),
            dma((2,)),
            dma((half, CUTS)),
            dma,
            dma((CUTS,)),
            pltpu.SemaphoreType.REGULAR,
            pltpu.VMEM(pair.shape, pair.dtype),
            pltpu.VMEM((width, rows), pair_mask.dtype),
            pltpu.VMEM((1, in_gain.size), in_gain.dtype),
            pltpu.VMEM((1, in_bias.size), in_bias.dtype),
            pltpu.VMEM(proj_weight.shape, proj_weight.dtype),
            pltpu.VMEM(gate_weight.shape, gate_weight.dtype),
            pltpu.VMEM((1, out_gain.size), out_gain.dtype),
            pltpu.VMEM((1, out_bias.size), out_bias.dtype),
            pltpu.VMEM(out_weight.shape, out_weight.dtype),
            dma((9,)),
        ],
        compiler_params=pltpu.CompilerParams(collective_id=0, has_side_effects=True),
    )(
        pair,
        pair_mask.T,
        in_gain.reshape(1, -1),
        in_bias.reshape(1, -1),
        proj_weight,
        gate_weight,
        out_gain.reshape(1, -1),
        out_bias.reshape(1, -1),
        out_weight,
    )


def solution(mesh):
    nx, ny, nz = mesh.shape["gx"], mesh.shape["gy"], mesh.shape["gz"]
    plane = ny * nz

    def on_device(pair, *others):
        rows, width, channels = pair.shape
        hidden = others[3].shape[1] // 4
        fits = (
            width * plane == LANES
            and rows * nx == LANES
            and rows % width == 0
            and rows * width % LANES == 0
            and nx == 4
            and channels % LANES == 0
            and hidden % (8 * CUTS * plane) == 0
        )
        if fits:
            return fused(nx, ny, nz, pair, *others)
        return with_collectives(pair, *others)

    return jax.shard_map(
        on_device,
        mesh=mesh,
        in_specs=(
            P("gx", ("gy", "gz"), None),
            P("gx", ("gy", "gz")),
            P(),
            P(),
            P(),
            P(),
            P(),
            P(),
            P(),
        ),
        out_specs=P("gx", ("gy", "gz"), None),
        check_vma=False,
    )
```
